32 devices in a mesh: dp: 1 (over z), cp: 32 (over y, x, core).
Axes of the slice: x: 4, y: 4, z: 1, core: 2. Of those that a mesh axis runs over, the one named last changes fastest.
The devices are a block of a 4x4x8 slice.
Arguments:
- hidden: bfloat16 [16384, 2560], P(('dp', 'cp'))
- w_query: bfloat16 [6, 2560, 8, 256], replicated
- w_key: bfloat16 [6, 2560, 4, 256], replicated
- w_value: bfloat16 [6, 2560, 4, 256], replicated
- w_out: bfloat16 [6, 8, 256, 2560], replicated
Outputs:
- output: bfloat16 [16384, 2560], P(('dp', 'cp'))
All inputs are finite; a program needn't handle non-finite values.
Results may differ from the reference program's by a relative error of at most 0.0117122.
Values are sent between devices in bfloat16 or wider.
A program may use at most 768 MiB of HBM per device.

```python
import jax
import jax.numpy as jnp
from jax import lax

TOK_DEV = 512
NUM_CP = 32
D = 2560
HEADS = 8
KV_HEADS = 4
HEAD = 256
WINDOW = 1024
LAYERS = 6

SEQ_LEN = TOK_DEV * NUM_CP
GROUP_SIZE = HEADS // KV_HEADS
QUERY_BLOCK = min(64, TOK_DEV)
NUM_BLOCKS = SEQ_LEN // QUERY_BLOCK
EPS_NORM = 1e-6
NEG_BIG = -1e30


def setup_inputs(seed: int = 0, part: int = 0) -> dict:
    base_key = jax.random.key(seed)
    hidden_key = jax.random.fold_in(jax.random.fold_in(base_key, 1), part)
    weight_keys = jax.random.split(jax.random.fold_in(base_key, 2), 4)
    hidden = jax.random.normal(hidden_key, (SEQ_LEN, D), jnp.float32)
    w_query = jax.random.normal(weight_keys[0], (LAYERS, D, HEADS, HEAD), jnp.float32) * D ** -0.5
    w_key = jax.random.normal(weight_keys[1], (LAYERS, D, KV_HEADS, HEAD), jnp.float32) * D ** -0.5
    w_value = jax.random.normal(weight_keys[2], (LAYERS, D, KV_HEADS, HEAD), jnp.float32) * D ** -0.5
    w_out = jax.random.normal(weight_keys[3], (LAYERS, HEADS, HEAD, D), jnp.float32) * (HEADS * HEAD) ** -0.5
    return {
        "hidden": hidden.astype(jnp.bfloat16),
        "w_query": w_query.astype(jnp.bfloat16),
        "w_key": w_key.astype(jnp.bfloat16),
        "w_value": w_value.astype(jnp.bfloat16),
        "w_out": w_out.astype(jnp.bfloat16),
    }


def rms_normed(rows_in):
    widened = rows_in.astype(jnp.float32)
    return widened * lax.rsqrt(jnp.mean(widened * widened, axis=-1, keepdims=True) + EPS_NORM)


def project(normed, weight):
    flat = weight.reshape(weight.shape[0], weight.shape[1] * weight.shape[2])
    product = jnp.dot(normed, flat, preferred_element_type=jnp.float32)
    return product.astype(jnp.bfloat16).reshape(normed.shape[0], weight.shape[1], weight.shape[2])


def attend_block(q_block, key_rows, value_rows, query_pos, key_pos, windowed):
    grouped = q_block.astype(jnp.float32).reshape(QUERY_BLOCK, KV_HEADS, GROUP_SIZE, HEAD)
    scores = jnp.einsum("qhgd,khd->hgqk", grouped, key_rows) * HEAD ** -0.5
    allowed = (key_pos[None, :] <= query_pos[:, None]) & (key_pos[None, :] >= 0)
    if windowed:
        allowed = allowed & (key_pos[None, :] > query_pos[:, None] - WINDOW)
    scores = jnp.where(allowed, scores, NEG_BIG)
    row_max = jnp.max(scores, axis=-1, keepdims=True)
    weights = jnp.exp(scores - row_max)
    row_sum = jnp.sum(weights, axis=-1)
    rounded = weights.astype(jnp.bfloat16).astype(jnp.float32)
    attn_out = jnp.einsum("hgqk,khd->hgqd", rounded, value_rows) / row_sum[..., None]
    return jnp.transpose(attn_out, (2, 0, 1, 3)).reshape(QUERY_BLOCK, HEADS, HEAD).astype(jnp.bfloat16)


def attention_layer(hidden, weights, windowed):
    w_query, w_key, w_value, w_out = weights
    normed = rms_normed(hidden).astype(jnp.bfloat16)
    queries = project(normed, w_query)
    key_rows = project(normed, w_key).astype(jnp.float32)
    value_rows = project(normed, w_value).astype(jnp.float32)
    if windowed:
        zero_pad = jnp.zeros((WINDOW, KV_HEADS, HEAD), jnp.float32)
        key_rows = jnp.concatenate([zero_pad, key_rows], axis=0)
        value_rows = jnp.concatenate([zero_pad, value_rows], axis=0)

    def one_block(block_idx):
        start_row = block_idx * QUERY_BLOCK
        q_block = lax.dynamic_slice_in_dim(queries, start_row, QUERY_BLOCK)
        query_pos = start_row + jnp.arange(QUERY_BLOCK)
        if windowed:
            key_span = WINDOW + QUERY_BLOCK
            key_blk = lax.dynamic_slice_in_dim(key_rows, start_row, key_span)
            value_blk = lax.dynamic_slice_in_dim(value_rows, start_row, key_span)
            key_pos = start_row - WINDOW + jnp.arange(key_span)
        else:
            key_blk = key_rows
            value_blk = value_rows
            key_pos = jnp.arange(SEQ_LEN)
        return attend_block(q_block, key_blk, value_blk, query_pos, key_pos, windowed)

    attn_out = lax.map(one_block, jnp.arange(NUM_BLOCKS)).reshape(SEQ_LEN, HEADS * HEAD)
    update = jnp.dot(attn_out, w_out.reshape(HEADS * HEAD, D), preferred_element_type=jnp.float32)
    return (hidden.astype(jnp.float32) + rms_normed(update)).astype(jnp.bfloat16)


def output_order(hidden):
    halves = hidden.reshape(2, NUM_CP, TOK_DEV // 2, D)
    return jnp.stack([halves[0], halves[1, ::-1]], axis=1).reshape(SEQ_LEN, D)


def reference(hidden, w_query, w_key, w_value, w_out):
    def local_step(state_in, weights):
        return attention_layer(state_in, weights, True), None

    stacked = (w_query[:LAYERS - 1], w_key[:LAYERS - 1], w_value[:LAYERS - 1], w_out[:LAYERS - 1])
    hidden = lax.scan(local_step, hidden, stacked)[0]
    last_weights = (w_query[LAYERS - 1], w_key[LAYERS - 1], w_value[LAYERS - 1], w_out[LAYERS - 1])
    hidden = attention_layer(hidden, last_weights, False)
    return output_order(hidden)
```

```python
import functools

import jax
import jax.numpy as jnp
import numpy as np
from jax import lax
from jax.experimental import pallas as pl
from jax.experimental.pallas import tpu as pltpu
from jax.sharding import PartitionSpec as P

WINDOW = 1024
EPS_NORM = 1e-6
NEG_BIG = -1e30
LOG2E = 1.4426950408889634
MESH = pl.DeviceIdType.MESH
NT = (((1,), (1,)), ((), ()))


def rms_normed(rows_in):
    widened = rows_in.astype(jnp.float32)
    return widened * lax.rsqrt(jnp.mean(widened * widened, axis=-1, keepdims=True) + EPS_NORM)


def iota2(shape, dim):
    return lax.broadcasted_iota(jnp.int32, shape, dim)


def perm_matrix(heads):
    dn = 128 // heads
    row = np.arange(256)
    h, ct, d = row // (2 * dn), (row // dn) % 2, row % dn
    out = np.zeros((256, 256), np.float32)
    out[row, d * 2 * heads + ct * heads + h] = 1
    return jnp.asarray(out, jnp.bfloat16)


def relayout_kernel(heads, perm, w_in, w_out):
    dn = 128 // heads
    for b in range(w_in.shape[1] // 512):
        pair = jnp.concatenate([w_in[0, b * 512:b * 512 + 256, :], w_in[0, b * 512 + 256:b * 512 + 512, :]], axis=1)
        moved = jnp.dot(perm[...], pair, preferred_element_type=jnp.float32).astype(jnp.bfloat16)
        for h in range(heads):
            for ct in range(2):
                row, col = (h * 2 + ct) * dn, h * 256 + ct * 128
                for i in range(2):
                    d0 = (2 * b + i) * dn
                    w_out[0, d0:d0 + dn, col:col + 128] = moved[row:row + dn, i * 128:(i + 1) * 128]


def flat_heads(w):
    layers, width, heads, head = w.shape
    rows = w.reshape(layers, width, heads, 2, 128).transpose(0, 1, 3, 2, 4).reshape(layers, width * 2 * heads, 128)
    step = 512
    return pl.pallas_call(
        functools.partial(relayout_kernel, heads),
        grid=(layers, width // step),
        in_specs=[pl.BlockSpec((256, 256), lambda l, i: (0, 0)), pl.BlockSpec((1, step * 2 * heads, 128), lambda l, i: (l, i, 0))],
        out_specs=pl.BlockSpec((1, step, heads * head), lambda l, i: (l, i, 0)),
        out_shape=jax.ShapeDtypeStruct((layers, width, heads * head), w.dtype),
        name="flat_heads",
    )(perm_matrix(heads), rows)


def local_kernel(num_dev, num_layers, x_in, wq_hbm, wk_hbm, wv_hbm, wo_hbm, x_out,
                 n_s, q_s, own_s, halo_a, halo_b, o_s, acc, wkv_buf, wq_buf, wo_buf,
                 kv_sem, q_sem, o_sem, send_a, send_b, recv_a, recv_b, credit_a, credit_b):
    me = lax.axis_index("cp")
    odd = lax.rem(me, 2) == 1
    partner = jnp.where(odd, me - 1, me + 1)
    fwd = lax.rem(me + 2, num_dev)
    back = lax.rem(me + num_dev - 2, num_dev)
    rows, width = n_s.shape
    half = rows // 2
    kv_heads = own_s.shape[0]
    head = own_s.shape[-1]
    scale = head ** -0.5 * LOG2E
    chunk = 32

    barrier = pltpu.get_barrier_semaphore()
    for other in (fwd, back, partner):
        pl.semaphore_signal(barrier, inc=1, device_id={"cp": other}, device_id_type=MESH)
    pl.semaphore_wait(barrier, 3)

    def kv_copies(layer, h):
        slot = lax.rem(h, 2)
        cols = pl.ds(pl.multiple_of(h * head, head), head)
        return (pltpu.make_async_copy(wk_hbm.at[layer, :, cols], wkv_buf.at[slot, 0], kv_sem.at[slot, 0]),
                pltpu.make_async_copy(wv_hbm.at[layer, :, cols], wkv_buf.at[slot, 1], kv_sem.at[slot, 1]))

    def q_copy(layer, h):
        slot = lax.rem(h, 2)
        cols = pl.ds(pl.multiple_of(h * 2 * head, 2 * head), 2 * head)
        return pltpu.make_async_copy(wq_hbm.at[layer, :, cols], wq_buf.at[slot], q_sem.at[slot])

    def o_copy(layer, h):
        slot = lax.rem(h, 2)
        part = pl.ds(pl.multiple_of(h * 2 * head, 2 * head), 2 * head)
        return pltpu.make_async_copy(wo_hbm.at[layer, part], wo_buf.at[slot], o_sem.at[slot])

    def start_kv(layer, h):
        for copy in kv_copies(layer, h):
            copy.start()

    def prefetch(start, layer, h):
        @pl.when(h < kv_heads - 2)
        def _():
            start(layer, h + 2)

        @pl.when(jnp.logical_and(h >= kv_heads - 2, layer < num_layers - 1))
        def _():
            start(layer + 1, h + 2 - kv_heads)

    for h in range(2):
        start_kv(0, h)
        q_copy(0, h).start()
        o_copy(0, h).start()

    def send_own(parity, h):
        return pltpu.make_async_remote_copy(
            src_ref=own_s.at[h], dst_ref=halo_a.at[parity, h], send_sem=send_a.at[h], recv_sem=recv_a.at[parity, h],
            device_id={"cp": fwd}, device_id_type=MESH)

    def send_partner(parity, h, src):
        return pltpu.make_async_remote_copy(
            src_ref=src, dst_ref=halo_b.at[parity, h], send_sem=send_b.at[h], recv_sem=recv_b.at[parity, h],
            device_id={"cp": partner}, device_id_type=MESH)

    def norm_rows(i, carry):
        part = pl.ds(pl.multiple_of(i * chunk, chunk), chunk)
        n_s[part, :] = rms_normed(x_in[part, :]).astype(jnp.bfloat16)
        x_out[part, :] = x_in[part, :]
        return carry

    lax.fori_loop(0, rows // chunk, norm_rows, 0)

    bias_a = jnp.where(me < 2, NEG_BIG, 0.0)
    bias_b = jnp.where(me < 1, NEG_BIG, 0.0)

    def attend(parity, h, j):
        blocks = [(halo_a.at[parity, h], 0, bias_a), (halo_a.at[parity, h], 1, bias_a),
                  (halo_b.at[parity, h], 0, bias_b), (halo_b.at[parity, h], 1, bias_b),
                  (own_s.at[h], 0, None), (own_s.at[h], 1, None)][j:j + 5]
        q_tile = q_s[h, j]
        row = lax.rem(iota2((2 * half, half), 0), half)
        key = iota2((2 * half, half), 1)
        tiles = []
        for i, (ref, part, bias) in enumerate(blocks):
            keys = ref[0, part * half:(part + 1) * half, :]
            scores = lax.dot_general(q_tile, keys, NT, preferred_element_type=jnp.float32) * scale
            if bias is not None:
                scores = scores + bias
            if i == 0:
                scores = jnp.where(key > row, scores, NEG_BIG)
            if i == len(blocks) - 1:
                scores = jnp.where(key <= row, scores, NEG_BIG)
            tiles.append(scores)
        top = jnp.max(functools.reduce(jnp.maximum, tiles), axis=-1, keepdims=True)
        total, out = None, None
        for scores, (ref, part, _) in zip(tiles, blocks):
            e = jnp.exp2(scores - top)
            total = e if total is None else total + e
            term = jnp.dot(e.astype(jnp.bfloat16), ref[1, part * half:(part + 1) * half, :], preferred_element_type=jnp.float32)
            out = term if out is None else out + term
        out = (out / jnp.sum(total, axis=-1, keepdims=True)).astype(jnp.bfloat16)
        for g in range(2):
            o_s[j * half:(j + 1) * half, g * head:(g + 1) * head] = out[g * half:(g + 1) * half, :]

    def layer_step(layer, carry):
        parity = lax.rem(layer, 2)

        @pl.when(layer >= 2)
        def _():
            pl.semaphore_wait(credit_a, 1)
            pl.semaphore_wait(credit_b, 1)

        def kv_step(h, c):
            slot = lax.rem(h, 2)
            for copy in kv_copies(layer, h):
                copy.wait()
            for i in range(2):
                own_s[h, i] = jnp.dot(n_s[...], wkv_buf[slot, i], preferred_element_type=jnp.float32).astype(jnp.bfloat16)
            prefetch(start_kv, layer, h)
            send_own(parity, h).start()

            @pl.when(jnp.logical_not(odd))
            def _():
                send_partner(parity, h, own_s.at[h]).start()
            return c

        lax.fori_loop(0, kv_heads, kv_step, 0)

        def q_step(h, c):
            slot = lax.rem(h, 2)
            q_copy(layer, h).wait()
            for g in range(2):
                q = jnp.dot(n_s[...], wq_buf[slot, :, g * head:(g + 1) * head], preferred_element_type=jnp.float32).astype(jnp.bfloat16)
                for j in range(2):
                    q_s[h, j, g * half:(g + 1) * half, :] = q[j * half:(j + 1) * half, :]
            prefetch(lambda *a: q_copy(*a).start(), layer, h)
            return c

        lax.fori_loop(0, kv_heads, q_step, 0)

        def attn_step(h, c):
            slot = lax.rem(h, 2)
            send_own(parity, h).wait_recv()

            @pl.when(odd)
            def _():
                send_partner(parity, h, halo_a.at[parity, h]).start()
            send_partner(parity, h, own_s.at[h]).wait_recv()
            attend(parity, h, 0)
            attend(parity, h, 1)
            o_copy(layer, h).wait()

            def out_part(i, cc):
                cols = pl.ds(pl.multiple_of(i * 512, 512), 512)
                part = jnp.dot(o_s[...], wo_buf[slot, :, cols], preferred_element_type=jnp.float32)

                @pl.when(h == 0)
                def _():
                    acc[:, cols] = part

                @pl.when(h > 0)
                def _():
                    acc[:, cols] = acc[:, cols] + part
                return cc

            lax.fori_loop(0, width // 512, out_part, 0)
            prefetch(lambda *a: o_copy(*a).start(), layer, h)
            return c

        lax.fori_loop(0, kv_heads, attn_step, 0)

        def drain(h, c):
            send_own(parity, h).wait_send()
            send_partner(parity, h, own_s.at[h]).wait_send()
            return c

        lax.fori_loop(0, kv_heads, drain, 0)

        @pl.when(layer < num_layers - 2)
        def _():
            pl.semaphore_signal(credit_a, inc=1, device_id={"cp": back}, device_id_type=MESH)
            pl.semaphore_signal(credit_b, inc=1, device_id={"cp": partner}, device_id_type=MESH)

        def update_rows(i, c):
            part = pl.ds(pl.multiple_of(i * 16, 16), 16)
            new = (x_out[part, :].astype(jnp.float32) + rms_normed(acc[part, :])).astype(jnp.bfloat16)
            x_out[part, :] = new
            n_s[part, :] = rms_normed(new).astype(jnp.bfloat16)
            return c

        lax.fori_loop(0, rows // 16, update_rows, 0)
        return carry

    lax.fori_loop(0, num_layers, layer_step, 0)


def local_layers(hidden, w_query, w_key, w_value, w_out, num_dev, num_layers):
    rows, width = hidden.shape
    kv_width = w_key.shape[2]
    head = 256
    kv_heads = kv_width // head
    half = rows // 2
    bf16, f32 = jnp.bfloat16, jnp.float32
    hbm = pl.BlockSpec(memory_space=pltpu.HBM)
    vmem = pl.BlockSpec(memory_space=pltpu.VMEM)
    dma = pltpu.SemaphoreType.DMA
    return pl.pallas_call(
        functools.partial(local_kernel, num_dev, num_layers),
        out_shape=jax.ShapeDtypeStruct((rows, width), bf16),
        in_specs=[vmem, hbm, hbm, hbm, hbm],
        out_specs=vmem,
        scratch_shapes=[
            pltpu.VMEM((rows, width), bf16),
            pltpu.VMEM((kv_heads, 2, 2 * half, head), bf16),
            pltpu.VMEM((kv_heads, 2, rows, head), bf16),
            pltpu.VMEM((2, kv_heads, 2, rows, head), bf16),
            pltpu.VMEM((2, kv_heads, 2, rows, head), bf16),
            pltpu.VMEM((rows, 2 * head), bf16),
            pltpu.VMEM((rows, width), f32),
            pltpu.VMEM((2, 2, width, head), bf16),
            pltpu.VMEM((2, width, 2 * head), bf16),
            pltpu.VMEM((2, 2 * head, width), bf16),
            dma((2, 2)), dma((2,)), dma((2,)),
            dma((kv_heads,)), dma((kv_heads,)), dma((2, kv_heads)), dma((2, kv_heads)),
            pltpu.SemaphoreType.REGULAR, pltpu.SemaphoreType.REGULAR,
        ],
        compiler_params=pltpu.CompilerParams(collective_id=0, has_side_effects=True, vmem_limit_bytes=62 * 1024 * 1024),
        name="local_layers",
    )(hidden, w_query, w_key, w_value, w_out)


def flash_kernel(num_dev, q_ref, kv_hbm, out_ref, kv_buf, acc, m_s, l_s, sems):
    me = lax.axis_index("cp")
    half = q_ref.shape[1] // 2
    head = q_ref.shape[2]
    scale = head ** -0.5 * LOG2E
    num_rows = q_ref.shape[1]
    step_keys = kv_buf.shape[2]
    blocks = (me, 2 * num_dev - 1 - me)
    need = [(b * half + half + step_keys - 1) // step_keys for b in blocks]
    copies=lambda c: pltpu.make_async_copy(kv_hbm.at[c], kv_buf.at[c], sems.at[c])
    def start(c, carry):
        copies(c).start(); return carry
    lax.fori_loop(0, need[1], start, 0)
    m_s[...] = jnp.full(m_s.shape, NEG_BIG, jnp.float32)
    l_s[...] = jnp.zeros(l_s.shape, jnp.float32)
    acc[...] = jnp.zeros(acc.shape, jnp.float32)
    def one_tile(c, b, masked):
        s = lax.dot_general(q_ref[b], kv_buf[c, 0], NT, preferred_element_type=jnp.float32) * scale
        if masked:
            row = blocks[b] * half + lax.rem(iota2((num_rows, step_keys), 0), half)
            key = c * step_keys + iota2((num_rows, step_keys), 1)
            s = jnp.where(key <= row, s, NEG_BIG)
        old = m_s[b]
        top = jnp.maximum(old, jnp.max(s, axis=-1, keepdims=True))
        e = jnp.exp2(s - jnp.concatenate([top] * (step_keys // 128), axis=1))
        fix = jnp.exp2(old - top)
        m_s[b] = top
        part = e[:, 0:128]
        for i in range(1, step_keys // 128):
            part = part + e[:, i * 128:(i + 1) * 128]
        l_s[b] = l_s[b] * fix + part
        acc[b] = acc[b] * jnp.concatenate([fix] * (head // 128), axis=1) + jnp.dot(e.astype(jnp.bfloat16), kv_buf[c, 1], preferred_element_type=jnp.float32)
    def tile(c, b):
        edge = c == need[b] - 1
        @pl.when(edge)
        def _(): one_tile(c, b, True)
        @pl.when(jnp.logical_not(edge))
        def _(): one_tile(c, b, False)
    def body(c, carry):
        copies(c).wait()
        tile(c, 1)
        @pl.when(c < need[0])
        def _(): tile(c, 0)
        return carry
    lax.fori_loop(0, need[1], body, 0)
    for b in range(2):
        inv = 1.0 / jnp.sum(l_s[b],axis=-1,keepdims=True)
        out = (acc[b] * inv).astype(jnp.bfloat16)
        for g in range(2):
            out_ref[b * half:(b + 1) * half, g * head:(g + 1) * head] = out[g * half:(g + 1) * half]
def flash_head(queries, kv_all, num_dev):
    _, num_rows, head = queries.shape
    half = num_rows // 2
    f32 = jnp.float32
    nch=kv_all.shape[0]; tok = kv_all.shape[2]
    return pl.pallas_call(
        functools.partial(flash_kernel, num_dev),
        out_shape=jax.ShapeDtypeStruct((2 * half, 2 * head), jnp.bfloat16),
        in_specs=[pl.BlockSpec(memory_space=pltpu.VMEM), pl.BlockSpec(memory_space=pltpu.HBM)],
        out_specs=pl.BlockSpec(memory_space=pltpu.VMEM),
        scratch_shapes=[pltpu.VMEM((nch, 2, tok, head), jnp.bfloat16), pltpu.VMEM((2, num_rows, head), f32),
            pltpu.VMEM((2, num_rows, 128), f32), pltpu.VMEM((2, num_rows, 128), f32), pltpu.SemaphoreType.DMA((nch,))],
        compiler_params=pltpu.CompilerParams(vmem_limit_bytes=48 * 1024 * 1024),
        cost_estimate=pl.CostEstimate(flops=20_000_000_000, bytes_accessed=16_000_000, transcendentals=0), name="flash_head")(queries, kv_all)


def output_owner(block_idx, num_dev):
    return block_idx if block_idx < num_dev else 2 * num_dev - 1 - block_idx


def to_output_layout(hidden, dev_rank, num_dev):
    block_len = hidden.shape[0] // 2
    even_pairs = [(source, output_owner(2 * source, num_dev)) for source in range(num_dev)]
    odd_pairs = [(source, output_owner(2 * source + 1, num_dev)) for source in range(num_dev)]
    from_even = lax.ppermute(hidden[:block_len], "cp", even_pairs)
    from_odd = lax.ppermute(hidden[block_len:], "cp", odd_pairs)
    is_even = dev_rank % 2 == 0
    lead_rows = jnp.where(is_even, from_even, from_odd)
    trail_rows = jnp.where(is_even, from_odd, from_even)
    return jnp.concatenate([lead_rows, trail_rows], axis=0)


def solution(mesh):
    num_dev = mesh.shape["cp"]

    def per_device(hidden, w_query, w_key, w_value, w_out):
        dev_rank = lax.axis_index("cp")
        layers, width, heads, head = w_query.shape
        kv_heads = w_key.shape[2]
        group = heads // kv_heads
        wq = flat_heads(w_query)
        wk = flat_heads(w_key)
        wv = flat_heads(w_value)
        wo = w_out.reshape(layers, heads * head, width)
        last = layers - 1
        hidden = local_layers(hidden, wq, wk, wv, wo, num_dev, last)
        rows = hidden.shape[0]
        half = rows // 2
        normed = rms_normed(hidden).astype(jnp.bfloat16)
        gathered = []
        for h in range(kv_heads):
            cols = slice(h * head, (h + 1) * head)
            k = jnp.dot(normed, wk[last][:, cols], preferred_element_type=jnp.float32).astype(jnp.bfloat16)
            v = jnp.dot(normed, wv[last][:, cols], preferred_element_type=jnp.float32).astype(jnp.bfloat16)
            gathered.append(lax.all_gather(jnp.stack([k, v]), "cp"))
        hidden = to_output_layout(hidden, dev_rank, num_dev)
        normed = rms_normed(hidden).astype(jnp.bfloat16)
        queries = jnp.dot(normed, wq[last], preferred_element_type=jnp.float32).astype(jnp.bfloat16)
        queries = queries.reshape(2, half, kv_heads, group, head)
        outs = []
        for h in range(kv_heads):
            q = jnp.transpose(queries[:, :, h], (0, 2, 1, 3)).reshape(2, group * half, head)
            outs.append(flash_head(q, gathered[h], num_dev))
        attn = jnp.concatenate(outs, axis=1)
        update = jnp.dot(attn, wo[last], preferred_element_type=jnp.float32)
        return (hidden.astype(jnp.float32) + rms_normed(update)).astype(jnp.bfloat16)

    row_spec = P(("dp", "cp"), None)
    return jax.shard_map(per_device, mesh=mesh, in_specs=(row_spec, P(), P(), P(), P()), out_specs=row_spec, check_vma=False)
```

```python
import functools

import jax
import jax.numpy as jnp
import numpy as np
from jax import lax
from jax.experimental import pallas as pl
from jax.experimental.pallas import tpu as pltpu
from jax.sharding import PartitionSpec as P


EPS_NORM = 1e-6
NEG_BIG = -1e30
LOG2E = 1.4426950408889634
MESH = pl.DeviceIdType.MESH
NT = (((1,), (1,)), ((), ()))


def rms_normed(rows_in):
    widened = rows_in.astype(jnp.float32)
    return widened * lax.rsqrt(jnp.mean(widened * widened, axis=-1, keepdims=True) + EPS_NORM)


def iota2(shape, dim):
    return lax.broadcasted_iota(jnp.int32, shape, dim)


def perm_matrix(heads):
    dn = 128 // heads
    row = np.arange(256)
    h, ct, d = row // (2 * dn), (row // dn) % 2, row % dn
    out = np.zeros((256, 256), np.float32)
    out[row, d * 2 * heads + ct * heads + h] = 1
    return jnp.asarray(out, jnp.bfloat16)


def local_kernel(num_dev, num_layers, x_hbm, wq_hbm, wk_hbm, wv_hbm, wo_hbm, perm_q, perm_k, x_out, own_s,
                 n_s, q_s, halo_a, halo_b, o_s, acc, w_s, raw, wo_buf,
                 x_sem, raw_sem, o_sem, send_a, send_b, recv_a, recv_b, credit_a, credit_b):
    me = lax.axis_index("cp")
    odd = lax.rem(me, 2) == 1
    partner = jnp.where(odd, me - 1, me + 1)
    fwd = lax.rem(me + 2, num_dev)
    back = lax.rem(me + num_dev - 2, num_dev)
    rows, width = n_s.shape
    half = rows // 2
    kv_heads = own_s.shape[0]
    heads = 2 * kv_heads
    head = own_s.shape[-1]
    scale = head ** -0.5 * LOG2E
    slots, raw_rows, lanes = raw.shape
    dq, dk = raw_rows // (2 * heads), raw_rows // (2 * kv_heads)
    kv_chunks, q_chunks = 2 * width // dk, width // dq
    span = kv_chunks + q_chunks
    total_chunks = span * num_layers + kv_chunks

    barrier = pltpu.get_barrier_semaphore()
    for other in (fwd, back, partner):
        pl.semaphore_signal(barrier, inc=1, device_id={"cp": other}, device_id_type=MESH)
    pl.semaphore_wait(barrier, 3)

    def raw_copy(src, layer, i, g):
        slot = lax.rem(g, slots)
        part = pl.ds(pl.multiple_of(i * raw_rows, raw_rows), raw_rows)
        return pltpu.make_async_copy(src.at[layer, part], raw.at[slot], raw_sem.at[slot])

    def start_chunk(g):
        layer, i = g // span, lax.rem(g, span)

        @pl.when(jnp.logical_and(g < total_chunks, i < kv_chunks // 2))
        def _():
            raw_copy(wk_hbm, layer, i, g).start()

        @pl.when(jnp.logical_and(g < total_chunks, jnp.logical_and(i >= kv_chunks // 2, i < kv_chunks)))
        def _():
            raw_copy(wv_hbm, layer, i - kv_chunks // 2, g).start()

        @pl.when(jnp.logical_and(g < total_chunks, i >= kv_chunks))
        def _():
            raw_copy(wq_hbm, layer, i - kv_chunks, g).start()

    def flatten_chunk(layer, i, is_q):
        g = layer * span + i + (kv_chunks if is_q else 0)
        slot = lax.rem(g, slots)
        raw_copy(wk_hbm, 0, 0, g).wait()
        perm = perm_q if is_q else perm_k
        planes = heads if is_q else kv_heads
        dn = lanes // planes
        base = i * dq if is_q else lax.rem(i, kv_chunks // 2) * dk
        shift = 0 if is_q else pl.multiple_of(i // (kv_chunks // 2) * head, head)
        for b in range(raw_rows // 512):
            pair = jnp.concatenate([raw[slot, b * 512:b * 512 + 256, :], raw[slot, b * 512 + 256:b * 512 + 512, :]], axis=1)
            moved = jnp.dot(perm[...], pair, preferred_element_type=jnp.float32).astype(jnp.bfloat16)
            for h in range(planes):
                for ct in range(2):
                    row = (h * 2 + ct) * dn
                    for k in range(2):
                        part = pl.ds(pl.multiple_of(base + (2 * b + k) * dn, dn), dn)
                        piece = moved[row:row + dn, k * lanes:(k + 1) * lanes]
                        if is_q:
                            col = h % 2 * head + ct * lanes
                            w_s[h // 2, part, col:col + lanes] = piece
                        else:
                            w_s[h, part, pl.ds(pl.multiple_of(shift + ct * lanes, lanes), lanes)] = piece
        start_chunk(g + slots)

    def o_copy(layer, h):
        slot = lax.rem(h, 2)
        part = pl.ds(pl.multiple_of(h * 2 * head, 2 * head), 2 * head)
        return pltpu.make_async_copy(wo_hbm.at[layer, part], wo_buf.at[slot], o_sem.at[slot])

    x_copy = pltpu.make_async_copy(x_hbm, x_out, x_sem)
    x_copy.start()
    for g in range(slots):
        start_chunk(jnp.int32(g))
    for h in range(2):
        o_copy(0, h).start()

    def send_own(parity, h):
        return pltpu.make_async_remote_copy(
            src_ref=own_s.at[h], dst_ref=halo_a.at[parity, h], send_sem=send_a.at[h], recv_sem=recv_a.at[parity, h],
            device_id={"cp": fwd}, device_id_type=MESH)

    def send_partner(parity, h, src):
        return pltpu.make_async_remote_copy(
            src_ref=src, dst_ref=halo_b.at[parity, h], send_sem=send_b.at[h], recv_sem=recv_b.at[parity, h],
            device_id={"cp": partner}, device_id_type=MESH)

    def flatten_range(layer, lo, hi, is_q):
        def one(i, c):
            flatten_chunk(layer, i, is_q)
            return c

        lax.fori_loop(lo, hi, one, 0)

    x_copy.wait()

    def norm_rows(i, carry):
        part = pl.ds(pl.multiple_of(i * 32, 32), 32)
        n_s[part, :] = rms_normed(x_out[part, :]).astype(jnp.bfloat16)
        return carry

    lax.fori_loop(0, rows // 32, norm_rows, 0)
    flatten_range(0, 0, kv_chunks, False)

    bias_a = jnp.where(me < 2, NEG_BIG, 0.0)
    bias_b = jnp.where(me < 1, NEG_BIG, 0.0)

    def attend(parity, h, j):
        blocks = [(halo_a.at[parity, h], 0, bias_a), (halo_a.at[parity, h], 1, bias_a),
                  (halo_b.at[parity, h], 0, bias_b), (halo_b.at[parity, h], 1, bias_b),
                  (own_s.at[h], 0, None), (own_s.at[h], 1, None)][j:j + 5]
        q_tile = q_s[h, j]
        row = lax.rem(iota2((2 * half, half), 0), half)
        key = iota2((2 * half, half), 1)
        tiles = []
        for i, (ref, part, bias) in enumerate(blocks):
            keys = ref[0, part * half:(part + 1) * half, :]
            scores = lax.dot_general(q_tile, keys, NT, preferred_element_type=jnp.float32) * scale
            if bias is not None:
                scores = scores + bias
            if i == 0:
                scores = jnp.where(key > row, scores, NEG_BIG)
            if i == len(blocks) - 1:
                scores = jnp.where(key <= row, scores, NEG_BIG)
            tiles.append(scores)
        top = jnp.max(functools.reduce(jnp.maximum, tiles), axis=-1, keepdims=True)
        total, out = None, None
        for scores, (ref, part, _) in zip(tiles, blocks):
            e = jnp.exp2(scores - top)
            total = e if total is None else total + e
            term = jnp.dot(e.astype(jnp.bfloat16), ref[1, part * half:(part + 1) * half, :], preferred_element_type=jnp.float32)
            out = term if out is None else out + term
        out = (out / jnp.sum(total, axis=-1, keepdims=True)).astype(jnp.bfloat16)
        for g in range(2):
            o_s[j * half:(j + 1) * half, g * head:(g + 1) * head] = out[g * half:(g + 1) * half, :]

    def project_kv(h):
        kv = jnp.dot(n_s[...], w_s[h], preferred_element_type=jnp.float32).astype(jnp.bfloat16)
        own_s[h, 0] = kv[:, 0:head]
        own_s[h, 1] = kv[:, head:2 * head]

    def layer_step(layer, carry):
        parity = lax.rem(layer, 2)

        @pl.when(layer >= 2)
        def _():
            pl.semaphore_wait(credit_a, 1)
            pl.semaphore_wait(credit_b, 1)

        def kv_step(h, c):
            project_kv(h)
            send_own(parity, h).start()

            @pl.when(jnp.logical_not(odd))
            def _():
                send_partner(parity, h, own_s.at[h]).start()

            return c

        lax.fori_loop(0, kv_heads, kv_step, 0)
        flatten_range(layer, 0, q_chunks, True)

        def q_step(h, c):
            q = jnp.dot(n_s[...], w_s[h], preferred_element_type=jnp.float32).astype(jnp.bfloat16)
            for g in range(2):
                for j in range(2):
                    q_s[h, j, g * half:(g + 1) * half, :] = q[j * half:(j + 1) * half, g * head:(g + 1) * head]
            return c

        lax.fori_loop(0, kv_heads, q_step, 0)

        def attn_step(h, c):
            slot = lax.rem(h, 2)
            send_own(parity, h).wait_recv()

            @pl.when(odd)
            def _():
                send_partner(parity, h, halo_a.at[parity, h]).start()

            flatten_range(layer + 1, h * kv_chunks // kv_heads, (h + 1) * kv_chunks // kv_heads, False)
            send_partner(parity, h, own_s.at[h]).wait_recv()
            attend(parity, h, 0)
            attend(parity, h, 1)
            o_copy(layer, h).wait()

            def out_part(i, cc):
                cols = pl.ds(pl.multiple_of(i * 512, 512), 512)
                part = jnp.dot(o_s[...], wo_buf[slot, :, cols], preferred_element_type=jnp.float32)

                @pl.when(h == 0)
                def _():
                    acc[:, cols] = part

                @pl.when(h > 0)
                def _():
                    acc[:, cols] = acc[:, cols] + part

                return cc

            lax.fori_loop(0, width // 512, out_part, 0)

            @pl.when(h < kv_heads - 2)
            def _():
                o_copy(layer, h + 2).start()

            @pl.when(jnp.logical_and(h >= kv_heads - 2, layer < num_layers - 1))
            def _():
                o_copy(layer + 1, h + 2 - kv_heads).start()

            return c

        lax.fori_loop(0, kv_heads, attn_step, 0)

        def drain(h, c):
            send_own(parity, h).wait_send()
            send_partner(parity, h, own_s.at[h]).wait_send()
            return c

        lax.fori_loop(0, kv_heads, drain, 0)

        @pl.when(layer < num_layers - 2)
        def _():
            pl.semaphore_signal(credit_a, inc=1, device_id={"cp": back}, device_id_type=MESH)
            pl.semaphore_signal(credit_b, inc=1, device_id={"cp": partner}, device_id_type=MESH)

        def update_rows(i, c):
            part = pl.ds(pl.multiple_of(i * 32, 32), 32)
            fresh = (x_out[part, :].astype(jnp.float32) + rms_normed(acc[part, :])).astype(jnp.bfloat16)
            x_out[part, :] = fresh
            n_s[part, :] = rms_normed(fresh).astype(jnp.bfloat16)
            return c

        lax.fori_loop(0, rows // 32, update_rows, 0)
        return carry

    lax.fori_loop(0, num_layers, layer_step, 0)

    def last_kv(h, c):
        project_kv(h)
        return c

    lax.fori_loop(0, kv_heads, last_kv, 0)


def tile_rows(w):
    layers, width, heads, _ = w.shape
    return w.reshape(layers, width, heads, 2, 128).transpose(0, 1, 3, 2, 4).reshape(layers, width * 2 * heads, 128)


def local_layers(hidden, w_query, w_key, w_value, w_out, num_dev, num_layers):
    rows, width = hidden.shape
    heads, head = w_query.shape[2:]
    kv_heads = w_key.shape[2]
    half = rows // 2
    bf16, f32 = jnp.bfloat16, jnp.float32
    hbm = pl.BlockSpec(memory_space=pltpu.HBM)
    vmem = pl.BlockSpec(memory_space=pltpu.VMEM)
    dma = pltpu.SemaphoreType.DMA
    return pl.pallas_call(
        functools.partial(local_kernel, num_dev, num_layers),
        out_shape=(jax.ShapeDtypeStruct((rows, width), bf16), jax.ShapeDtypeStruct((kv_heads, 2, rows, head), bf16)),
        in_specs=[hbm, hbm, hbm, hbm, hbm, vmem, vmem],
        out_specs=(vmem, vmem),
        scratch_shapes=[
            pltpu.VMEM((rows, width), bf16),
            pltpu.VMEM((kv_heads, 2, 2 * half, head), bf16),
            pltpu.VMEM((2, kv_heads, 2, rows, head), bf16),
            pltpu.VMEM((2, kv_heads, 2, rows, head), bf16),
            pltpu.VMEM((rows, 2 * head), bf16),
            pltpu.VMEM((rows, width), f32),
            pltpu.VMEM((kv_heads, width, 2 * head), bf16),
            pltpu.VMEM((4, 4096, 128), bf16),
            pltpu.VMEM((2, 2 * head, width), bf16),
            dma, dma((4,)), dma((2,)),
            dma((kv_heads,)), dma((kv_heads,)), dma((2, kv_heads)), dma((2, kv_heads)),
            pltpu.SemaphoreType.REGULAR, pltpu.SemaphoreType.REGULAR,
        ],
        compiler_params=pltpu.CompilerParams(collective_id=0, has_side_effects=True, vmem_limit_bytes=62 * 1024 * 1024),
        name="local_layers",
    )(hidden, tile_rows(w_query), tile_rows(w_key), tile_rows(w_value), w_out, perm_matrix(heads), perm_matrix(kv_heads))


def output_kernel(attn, w, x, out, acc):
    i = pl.program_id(0)
    part = jnp.dot(attn[...], w[0], preferred_element_type=jnp.float32)

    @pl.when(i == 0)
    def _():
        acc[...] = part

    @pl.when(i > 0)
    def _():
        acc[...] = acc[...] + part

    @pl.when(i == pl.num_programs(0) - 1)
    def _():
        out[...] = (x[...].astype(jnp.float32) + rms_normed(acc[...])).astype(jnp.bfloat16)


def output_update(hidden, outs, w_out, layer):
    rows, width = hidden.shape
    attn = jnp.concatenate(outs, axis=1)
    depth = attn.shape[1] // 4
    return pl.pallas_call(
        output_kernel,
        grid=(4,),
        in_specs=[pl.BlockSpec((rows, depth), lambda i: (0, i)), pl.BlockSpec((1, depth, width), lambda i: (layer, i, 0)),
                  pl.BlockSpec((rows, width), lambda i: (0, 0))],
        out_specs=pl.BlockSpec((rows, width), lambda i: (0, 0)),
        out_shape=jax.ShapeDtypeStruct((rows, width), jnp.bfloat16),
        scratch_shapes=[pltpu.VMEM((rows, width), jnp.float32)],
        name="output_update",
    )(attn, w_out, hidden)


def flash_kernel(num_dev, which, q_ref, kv_hbm, out_ref, kv_buf, acc, m_s, l_s, s_a, s_b, sems):
    nch = kv_buf.shape[0]
    me = lax.axis_index("cp")
    half = q_ref.shape[1] // 2
    head = q_ref.shape[2]
    scale = head ** -0.5 * LOG2E
    num_rows = q_ref.shape[1]
    step_keys = kv_buf.shape[2]
    blocks = (me, 2 * num_dev - 1 - me)
    need = [(b * half + half + step_keys - 1) // step_keys for b in blocks]
    copies=lambda c: pltpu.make_async_copy(kv_hbm.at[c, which], kv_buf.at[c], sems.at[c])

    def start(c, carry):
        copies(c).start(); return carry

    lax.fori_loop(0, need[1], start, 0)
    m_s[...] = jnp.full(m_s.shape, NEG_BIG, jnp.float32)
    l_s[...] = jnp.zeros(l_s.shape, jnp.float32)
    acc[...] = jnp.zeros(acc.shape, jnp.float32)
    total = num_dev + 1

    def where(t):
        trail = t < need[1]
        b = jnp.where(trail, 1, 0)
        c = jnp.where(trail, t, t - need[1])
        return b, jnp.minimum(c, nch - 1)

    def qk(t, dst):
        b, c = where(t)
        dst[...] = lax.dot_general(q_ref[b], kv_buf[c, 0], NT, preferred_element_type=jnp.float32) * scale

    def soft(t, src, nxt, dst, masked):
        if dst is not None:
            qk(nxt, dst)
        b, c = where(t)
        s = src[...]
        if masked:
            row = jnp.where(b == 1, blocks[1], blocks[0]) * half + lax.rem(iota2((num_rows, step_keys), 0), half)
            key = c * step_keys + iota2((num_rows, step_keys), 1)
            s = jnp.where(key <= row, s, NEG_BIG)
        old = m_s[b]
        top = jnp.maximum(old, jnp.max(s, axis=-1, keepdims=True))
        e = jnp.exp2(s - jnp.concatenate([top] * (step_keys // 128), axis=1))
        fix = jnp.exp2(old - top)
        m_s[b] = top
        part = e[:, 0:128]
        for i in range(1, step_keys // 128):
            part = part + e[:, i * 128:(i + 1) * 128]
        l_s[b] = l_s[b] * fix + part
        acc[b] = acc[b] * jnp.concatenate([fix] * (head // 128), axis=1) + jnp.dot(e.astype(jnp.bfloat16), kv_buf[c, 1], preferred_element_type=jnp.float32)

    def tile(t, src, dst):
        nxt = t + 1

        @pl.when(nxt < need[1])
        def _():
            copies(nxt).wait()

        edge = jnp.logical_or(t == need[1] - 1, t == total - 1)

        @pl.when(edge)
        def _():
            soft(t, src, nxt, dst, True)

        @pl.when(jnp.logical_not(edge))
        def _():
            soft(t, src, nxt, dst, False)

    copies(0).wait()
    qk(0, s_a)

    def pair(u, carry):
        tile(2 * u, s_a, s_b)
        tile(2 * u + 1, s_b, s_a)
        return carry

    lax.fori_loop(0, (total - 1) // 2, pair, 0)
    soft(total - 1, s_a, None, None, True)
    for b in range(2):
        inv = 1.0 / jnp.sum(l_s[b],axis=-1,keepdims=True)
        out = (acc[b] * inv).astype(jnp.bfloat16)
        for g in range(2):
            out_ref[b * half:(b + 1) * half, g * head:(g + 1) * head] = out[g * half:(g + 1) * half]


def flash_head(queries, kv_all, which, num_dev):
    _, num_rows, head = queries.shape
    half = num_rows // 2
    f32 = jnp.float32
    nch, tok = kv_all.shape[0], kv_all.shape[3]
    return pl.pallas_call(
        functools.partial(flash_kernel, num_dev, which),
        out_shape=jax.ShapeDtypeStruct((2 * half, 2 * head), jnp.bfloat16),
        in_specs=[pl.BlockSpec(memory_space=pltpu.VMEM), pl.BlockSpec(memory_space=pltpu.HBM)],
        out_specs=pl.BlockSpec(memory_space=pltpu.VMEM),
        scratch_shapes=[pltpu.VMEM((nch, 2, tok, head), jnp.bfloat16), pltpu.VMEM((2, num_rows, head), f32),
            pltpu.VMEM((2, num_rows, 128), f32), pltpu.VMEM((2, num_rows, 128), f32), pltpu.VMEM((num_rows, tok), f32), pltpu.VMEM((num_rows, tok), f32), pltpu.SemaphoreType.DMA((nch,))],
        compiler_params=pltpu.CompilerParams(vmem_limit_bytes=48 * 1024 * 1024),
        cost_estimate=pl.CostEstimate(flops=20_000_000_000, bytes_accessed=16_000_000, transcendentals=0), name="flash_head")(queries, kv_all)


def output_owner(block_idx, num_dev):
    return block_idx if block_idx < num_dev else 2 * num_dev - 1 - block_idx


def to_output_layout(hidden, dev_rank, num_dev):
    block_len = hidden.shape[0] // 2
    even_pairs = [(source, output_owner(2 * source, num_dev)) for source in range(num_dev)]
    odd_pairs = [(source, output_owner(2 * source + 1, num_dev)) for source in range(num_dev)]
    from_even = lax.ppermute(hidden[:block_len], "cp", even_pairs)
    from_odd = lax.ppermute(hidden[block_len:], "cp", odd_pairs)
    is_even = dev_rank % 2 == 0
    lead_rows = jnp.where(is_even, from_even, from_odd)
    trail_rows = jnp.where(is_even, from_odd, from_even)
    return jnp.concatenate([lead_rows, trail_rows], axis=0)


def solution(mesh):
    num_dev = mesh.shape["cp"]

    def per_device(hidden, w_query, w_key, w_value, w_out):
        dev_rank = lax.axis_index("cp")
        layers, width, heads, head = w_query.shape
        kv_heads = w_key.shape[2]
        group = heads // kv_heads
        wo = w_out.reshape(layers, heads * head, width)
        last = layers - 1
        hidden, kv = local_layers(hidden, w_query, w_key, w_value, wo, num_dev, last)
        half = hidden.shape[0] // 2
        cuts = [0, kv_heads - 1, kv_heads]
        most = lax.all_gather(kv[:cuts[1]], "cp")
        rest = lax.all_gather(kv[cuts[1]:], "cp")
        hidden = to_output_layout(hidden, dev_rank, num_dev)
        gathered = [most, rest]
        normed = rms_normed(hidden).astype(jnp.bfloat16)
        queries = jnp.einsum("td,dhe->the", normed, w_query[last], preferred_element_type=jnp.float32).astype(jnp.bfloat16)
        queries = queries.reshape(2, half, kv_heads, group, head)
        outs = []
        for lo, hi, kv_all in zip(cuts, cuts[1:], gathered):
            for h in range(lo, hi):
                q = jnp.transpose(queries[:, :, h], (0, 2, 1, 3)).reshape(2, group * half, head)
                outs.append(flash_head(q, kv_all, h - lo, num_dev))
        return output_update(hidden, outs, wo, last)

    row_spec = P(("dp", "cp"), None)
    return jax.shard_map(per_device, mesh=mesh, in_specs=(row_spec, P(), P(), P(), P()), out_specs=row_spec, check_vma=False)
```

```python
import functools
import math

import jax
import jax.numpy as jnp
import numpy as np
from jax import lax
from jax.experimental import pallas as pl
from jax.experimental.pallas import tpu as pltpu
from jax.sharding import PartitionSpec as P


EPS_NORM = 1e-6
NEG_BIG = -1e30
LOG2E = 1.4426950408889634
MESH = pl.DeviceIdType.MESH
NT = (((1,), (1,)), ((), ()))


def rms_normed(rows_in):
    widened = rows_in.astype(jnp.float32)
    return widened * lax.rsqrt(jnp.mean(widened * widened, axis=-1, keepdims=True) + EPS_NORM)


def iota2(shape, dim):
    return lax.broadcasted_iota(jnp.int32, shape, dim)


def perm_matrix(heads):
    dn = 128 // heads
    row = np.arange(256)
    h, ct, d = row // (2 * dn), (row // dn) % 2, row % dn
    out = np.zeros((256, 256), np.float32)
    out[row, d * 2 * heads + ct * heads + h] = 1
    return jnp.asarray(out, jnp.bfloat16)


def local_kernel(num_dev, num_layers, x_hbm, wq_hbm, wk_hbm, wv_hbm, wo_hbm, perm_q, perm_k, x_out, own_s,
                 n_s, q_s, halo_a, halo_b, o_s, acc, w_s, raw, wo_buf, relay_1, relay_2, s_a, s_b,
                 x_sem, raw_sem, o_sem, send_a, send_b, recv_a, recv_b, send_r, recv_r, credit_a, credit_b, credit_r, credit_t):
    me = lax.axis_index("cp")
    odd = lax.rem(me, 2) == 1
    partner = jnp.where(odd, me - 1, me + 1)
    fwd = lax.rem(me + 2, num_dev)
    back = lax.rem(me + num_dev - 2, num_dev)
    ring = math.isqrt(num_dev // 2)
    chips = num_dev // 2
    chip, core = me // 2, lax.rem(me, 2)

    def ring_dev(c, shift):
        base = c // ring * ring
        return 2 * (base + lax.rem(c - base + ring + shift, ring)) + core

    left, right = ring_dev(chip, -1), ring_dev(chip, 1)
    target = 2 * lax.rem(ring_dev(chip, 2) // 2 + 1, chips) + core
    writer = ring_dev(lax.rem(chip + chips - 1, chips), -2)
    rows, width = n_s.shape
    half = rows // 2
    kv_heads = own_s.shape[0]
    relayed = kv_heads - 1
    heads = 2 * kv_heads
    head = own_s.shape[-1]
    scale = head ** -0.5 * LOG2E
    slots, raw_rows, lanes = raw.shape
    dq, dk = raw_rows // (2 * heads), raw_rows // (2 * kv_heads)
    kv_chunks, q_chunks = 2 * width // dk, width // dq
    span = kv_chunks + q_chunks
    total_chunks = span * num_layers + kv_chunks

    barrier = pltpu.get_barrier_semaphore()
    for other in (fwd, back, partner, left, right, target, writer):
        pl.semaphore_signal(barrier, inc=1, device_id={"cp": other}, device_id_type=MESH)
    pl.semaphore_wait(barrier, 7)

    def raw_copy(src, layer, i, g):
        slot = lax.rem(g, slots)
        part = pl.ds(pl.multiple_of(i * raw_rows, raw_rows), raw_rows)
        return pltpu.make_async_copy(src.at[layer, part], raw.at[slot], raw_sem.at[slot])

    def start_chunk(g):
        layer, i = g // span, lax.rem(g, span)

        @pl.when(jnp.logical_and(g < total_chunks, i < kv_chunks // 2))
        def _():
            raw_copy(wk_hbm, layer, i, g).start()

        @pl.when(jnp.logical_and(g < total_chunks, jnp.logical_and(i >= kv_chunks // 2, i < kv_chunks)))
        def _():
            raw_copy(wv_hbm, layer, i - kv_chunks // 2, g).start()

        @pl.when(jnp.logical_and(g < total_chunks, i >= kv_chunks))
        def _():
            raw_copy(wq_hbm, layer, i - kv_chunks, g).start()

    def flatten_chunk(layer, i, is_q):
        g = layer * span + i + (kv_chunks if is_q else 0)
        slot = lax.rem(g, slots)
        raw_copy(wk_hbm, 0, 0, g).wait()
        perm = perm_q if is_q else perm_k
        planes = heads if is_q else kv_heads
        dn = lanes // planes
        base = i * dq if is_q else lax.rem(i, kv_chunks // 2) * dk
        shift = 0 if is_q else pl.multiple_of(i // (kv_chunks // 2) * head, head)
        for b in range(raw_rows // 512):
            pair = jnp.concatenate([raw[slot, b * 512:b * 512 + 256, :], raw[slot, b * 512 + 256:b * 512 + 512, :]], axis=1)
            moved = jnp.dot(perm[...], pair, preferred_element_type=jnp.float32).astype(jnp.bfloat16)
            for h in range(planes):
                for ct in range(2):
                    row = (h * 2 + ct) * dn
                    for k in range(2):
                        part = pl.ds(pl.multiple_of(base + (2 * b + k) * dn, dn), dn)
                        piece = moved[row:row + dn, k * lanes:(k + 1) * lanes]
                        if is_q:
                            col = h % 2 * head + ct * lanes
                            w_s[h // 2, part, col:col + lanes] = piece
                        else:
                            w_s[h, part, pl.ds(pl.multiple_of(shift + ct * lanes, lanes), lanes)] = piece
        start_chunk(g + slots)

    def head_at(i):
        return jnp.where(i < kv_heads - 2, i, 2 * kv_heads - 3 - i)

    def o_copy(layer, i):
        slot = lax.rem(i, 2)
        part = pl.ds(pl.multiple_of(head_at(i) * 2 * head, 2 * head), 2 * head)
        return pltpu.make_async_copy(wo_hbm.at[layer, part], wo_buf.at[slot], o_sem.at[slot])

    x_copy = pltpu.make_async_copy(x_hbm, x_out, x_sem)
    x_copy.start()
    for g in range(slots):
        start_chunk(jnp.int32(g))
    for i in range(2):
        o_copy(0, jnp.int32(i)).start()

    def send_own(parity, h):
        return pltpu.make_async_remote_copy(
            src_ref=own_s.at[h], dst_ref=halo_a.at[parity, h], send_sem=send_a.at[h], recv_sem=recv_a.at[parity, h],
            device_id={"cp": fwd}, device_id_type=MESH)

    def send_partner(parity, h, src):
        return pltpu.make_async_remote_copy(
            src_ref=src, dst_ref=halo_b.at[parity, h], send_sem=send_b.at[h], recv_sem=recv_b.at[parity, h],
            device_id={"cp": partner}, device_id_type=MESH)

    def hop(parity, leg, kv):
        src = (own_s.at[relayed, kv], relay_1.at[parity, kv], relay_2.at[parity, kv])[leg]
        dst = (relay_1.at[parity, kv], relay_2.at[parity, kv], halo_a.at[parity, relayed, kv])[leg]
        return pltpu.make_async_remote_copy(
            src_ref=src, dst_ref=dst, send_sem=send_r.at[leg, kv], recv_sem=recv_r.at[parity, leg, kv],
            device_id={"cp": (left, left, target)[leg]}, device_id_type=MESH)

    def pass_on(parity, leg, kv):
        hop(parity, leg, kv).wait_recv()
        hop(parity, leg + 1, kv).start()

    def flatten_range(layer, lo, hi, is_q):
        def one(i, c):
            flatten_chunk(layer, i, is_q)
            return c

        lax.fori_loop(lo, hi, one, 0)

    x_copy.wait()

    def norm_rows(i, carry):
        part = pl.ds(pl.multiple_of(i * 32, 32), 32)
        n_s[part, :] = rms_normed(x_out[part, :]).astype(jnp.bfloat16)
        return carry

    lax.fori_loop(0, rows // 32, norm_rows, 0)
    flatten_range(0, 0, kv_chunks, False)

    bias_a = jnp.where(me < 2, NEG_BIG, 0.0)
    bias_b = jnp.where(me < 1, NEG_BIG, 0.0)

    def attend(parity, h):
        row, key = iota2((half, half), 0), iota2((half, half), 1)
        units = [(j, g, (s_a, s_b)[j].at[g * half:(g + 1) * half]) for j in range(2) for g in range(2)]

        def blocks_of(j):
            return [(halo_a.at[parity, h], 0, bias_a), (halo_a.at[parity, h], 1, bias_a),
                    (halo_b.at[parity, h], 0, bias_b), (halo_b.at[parity, h], 1, bias_b),
                    (own_s.at[h], 0, None), (own_s.at[h], 1, None)][j:j + 5]

        def score(j, g, buf):
            q_tile = q_s[h, j, g * half:(g + 1) * half, :]
            for i, (ref, part, bias) in enumerate(blocks_of(j)):
                keys = ref[0, part * half:(part + 1) * half, :]
                scores = lax.dot_general(q_tile, keys, NT, preferred_element_type=jnp.float32) * scale
                if bias is not None:
                    scores = scores + bias
                if i == 0:
                    scores = jnp.where(key > row, scores, NEG_BIG)
                if i == 4:
                    scores = jnp.where(key <= row, scores, NEG_BIG)
                buf[:, i * half:(i + 1) * half] = scores

        score(*units[0])
        for u, (j, g, buf) in enumerate(units):
            if u + 1 < len(units):
                score(*units[u + 1])
            tiles = [buf[:, i * half:(i + 1) * half] for i in range(5)]
            top = jnp.max(functools.reduce(jnp.maximum, tiles), axis=-1, keepdims=True)
            total, out = None, None
            for scores, (ref, part, _) in zip(tiles, blocks_of(j)):
                e = jnp.exp2(scores - top)
                total = e if total is None else total + e
                term = jnp.dot(e.astype(jnp.bfloat16), ref[1, part * half:(part + 1) * half, :], preferred_element_type=jnp.float32)
                out = term if out is None else out + term
            out = (out / jnp.sum(total, axis=-1, keepdims=True)).astype(jnp.bfloat16)
            o_s[j * half:(j + 1) * half, g * head:(g + 1) * head] = out

    def project_kv(h):
        kv = jnp.dot(n_s[...], w_s[h], preferred_element_type=jnp.float32).astype(jnp.bfloat16)
        own_s[h, 0] = kv[:, 0:head]
        own_s[h, 1] = kv[:, head:2 * head]

    def layer_step(layer, carry):
        parity = lax.rem(layer, 2)

        @pl.when(layer >= 2)
        def _():
            pl.semaphore_wait(credit_a, 1)
            pl.semaphore_wait(credit_b, 1)
            pl.semaphore_wait(credit_r, 1)
            pl.semaphore_wait(credit_t, 1)

        def kv_step(i, c):
            h = lax.rem(i + relayed, kv_heads)
            project_kv(h)

            @pl.when(h == relayed)
            def _():
                hop(parity, 0, 0).start()
                hop(parity, 0, 1).start()

            @pl.when(h != relayed)
            def _():
                send_own(parity, h).start()

            @pl.when(jnp.logical_not(odd))
            def _():
                send_partner(parity, h, own_s.at[h]).start()

            return c

        lax.fori_loop(0, kv_heads, kv_step, 0)
        flatten_range(layer, 0, q_chunks // 2, True)
        pass_on(parity, 0, 0)
        flatten_range(layer, q_chunks // 2, q_chunks, True)

        def q_step(h, c):
            @pl.when(h == 1)
            def _():
                pass_on(parity, 0, 1)

            @pl.when(h == kv_heads - 1)
            def _():
                pass_on(parity, 1, 0)

            q = jnp.dot(n_s[...], w_s[h], preferred_element_type=jnp.float32).astype(jnp.bfloat16)
            for g in range(2):
                for j in range(2):
                    q_s[h, j, g * half:(g + 1) * half, :] = q[j * half:(j + 1) * half, g * head:(g + 1) * head]
            return c

        lax.fori_loop(0, kv_heads, q_step, 0)

        def attn_step(i, c):
            slot, h = lax.rem(i, 2), head_at(i)

            @pl.when(i == 1)
            def _():
                pass_on(parity, 1, 1)

            per = -(-kv_chunks // (kv_heads - 1))
            flatten_range(layer + 1, jnp.maximum(i - 1, 0) * per, jnp.minimum(i * per, kv_chunks), False)

            @pl.when(h == relayed)
            def _():
                hop(parity, 2, 0).wait_recv()
                hop(parity, 2, 1).wait_recv()

            @pl.when(h != relayed)
            def _():
                send_own(parity, h).wait_recv()

            @pl.when(odd)
            def _():
                send_partner(parity, h, halo_a.at[parity, h]).start()

            send_partner(parity, h, own_s.at[h]).wait_recv()
            attend(parity, h)
            o_copy(layer, i).wait()

            def out_part(t, cc):
                cols = pl.ds(pl.multiple_of(t * 512, 512), 512)
                part = jnp.dot(o_s[...], wo_buf[slot, :, cols], preferred_element_type=jnp.float32)

                @pl.when(i == 0)
                def _():
                    acc[:, cols] = part

                @pl.when(i > 0)
                def _():
                    acc[:, cols] = acc[:, cols] + part

                return cc

            lax.fori_loop(0, width // 512, out_part, 0)

            @pl.when(i < kv_heads - 2)
            def _():
                o_copy(layer, i + 2).start()

            @pl.when(jnp.logical_and(i >= kv_heads - 2, layer < num_layers - 1))
            def _():
                o_copy(layer + 1, i + 2 - kv_heads).start()

            return c

        lax.fori_loop(0, kv_heads, attn_step, 0)

        def drain(h, c):
            @pl.when(h != relayed)
            def _():
                send_own(parity, h).wait_send()

            send_partner(parity, h, own_s.at[h]).wait_send()
            return c

        lax.fori_loop(0, kv_heads, drain, 0)
        for leg in range(3):
            for kv in range(2):
                hop(parity, leg, kv).wait_send()

        @pl.when(layer < num_layers - 2)
        def _():
            pl.semaphore_signal(credit_a, inc=1, device_id={"cp": back}, device_id_type=MESH)
            pl.semaphore_signal(credit_b, inc=1, device_id={"cp": partner}, device_id_type=MESH)
            pl.semaphore_signal(credit_r, inc=1, device_id={"cp": right}, device_id_type=MESH)
            pl.semaphore_signal(credit_t, inc=1, device_id={"cp": writer}, device_id_type=MESH)

        def update_rows(i, c):
            part = pl.ds(pl.multiple_of(i * 32, 32), 32)
            fresh = (x_out[part, :].astype(jnp.float32) + rms_normed(acc[part, :])).astype(jnp.bfloat16)
            x_out[part, :] = fresh
            n_s[part, :] = rms_normed(fresh).astype(jnp.bfloat16)
            return c

        lax.fori_loop(0, rows // 32, update_rows, 0)
        return carry

    lax.fori_loop(0, num_layers, layer_step, 0)

    def last_kv(h, c):
        project_kv(h)
        return c

    lax.fori_loop(0, kv_heads, last_kv, 0)


def tile_rows(w):
    layers, width, heads, _ = w.shape
    return w.reshape(layers, width, heads, 2, 128).transpose(0, 1, 3, 2, 4).reshape(layers, width * 2 * heads, 128)


def local_layers(hidden, w_query, w_key, w_value, w_out, num_dev, num_layers):
    rows, width = hidden.shape
    heads, head = w_query.shape[2:]
    kv_heads = w_key.shape[2]
    half = rows // 2
    bf16, f32 = jnp.bfloat16, jnp.float32
    hbm = pl.BlockSpec(memory_space=pltpu.HBM)
    vmem = pl.BlockSpec(memory_space=pltpu.VMEM)
    dma = pltpu.SemaphoreType.DMA
    return pl.pallas_call(
        functools.partial(local_kernel, num_dev, num_layers),
        out_shape=(jax.ShapeDtypeStruct((rows, width), bf16), jax.ShapeDtypeStruct((kv_heads, 2, rows, head), bf16)),
        in_specs=[hbm, hbm, hbm, hbm, hbm, vmem, vmem],
        out_specs=(vmem, vmem),
        scratch_shapes=[
            pltpu.VMEM((rows, width), bf16),
            pltpu.VMEM((kv_heads, 2, 2 * half, head), bf16),
            pltpu.VMEM((2, kv_heads, 2, rows, head), bf16),
            pltpu.VMEM((2, kv_heads, 2, rows, head), bf16),
            pltpu.VMEM((rows, 2 * head), bf16),
            pltpu.VMEM((rows, width), f32),
            pltpu.VMEM((kv_heads, width, 2 * head), bf16),
            pltpu.VMEM((4, 4096, 128), bf16),
            pltpu.VMEM((2, 2 * head, width), bf16),
            pltpu.VMEM((2, 2, rows, head), bf16),
            pltpu.VMEM((2, 2, rows, head), bf16),
            pltpu.VMEM((2 * half, 5 * half), f32),
            pltpu.VMEM((2 * half, 5 * half), f32),
            dma, dma((4,)), dma((2,)),
            dma((kv_heads,)), dma((kv_heads,)), dma((2, kv_heads)), dma((2, kv_heads)), dma((3, 2)), dma((2, 3, 2)),
            pltpu.SemaphoreType.REGULAR, pltpu.SemaphoreType.REGULAR, pltpu.SemaphoreType.REGULAR, pltpu.SemaphoreType.REGULAR,
        ],
        compiler_params=pltpu.CompilerParams(collective_id=0, has_side_effects=True, vmem_limit_bytes=62 * 1024 * 1024),
        name="local_layers",
    )(hidden, tile_rows(w_query), tile_rows(w_key), tile_rows(w_value), w_out, perm_matrix(heads), perm_matrix(kv_heads))


def partial_kernel(count, *refs):
    attn, w, out = refs[:count], refs[count], refs[count + 1]
    for i in range(count):
        @pl.when(pl.program_id(0) == i)
        def _(i=i):
            part = jnp.dot(attn[i][...], w[0], preferred_element_type=jnp.float32)
            out[...] = part if i == 0 else out[...] + part


def final_kernel(attn, w, sofar, x, out, acc):
    acc[...] = sofar[...] + jnp.dot(attn[...], w[0], preferred_element_type=jnp.float32)

    def one(i, c):
        part = pl.ds(pl.multiple_of(i * 32, 32), 32)
        out[part, :] = (x[part, :].astype(jnp.float32) + rms_normed(acc[part, :])).astype(jnp.bfloat16)
        return c

    lax.fori_loop(0, out.shape[0] // 32, one, 0)


def partial_update(outs, w_out, layer):
    rows, depth = outs[0].shape
    width = w_out.shape[2]
    count = len(outs)
    return pl.pallas_call(
        functools.partial(partial_kernel, count),
        grid=(count,),
        in_specs=[pl.BlockSpec((rows, depth), lambda i: (0, 0))] * count + [pl.BlockSpec((1, depth, width), lambda i: (layer, i, 0))],
        out_specs=pl.BlockSpec((rows, width), lambda i: (0, 0)),
        out_shape=jax.ShapeDtypeStruct((rows, width), jnp.float32),
        cost_estimate=pl.CostEstimate(flops=2 * count * rows * depth * width, bytes_accessed=16_000_000, transcendentals=0),
        name="partial_update",
    )(*outs, w_out)


def final_update(hidden, sofar, last_out, w_out, layer):
    rows, width = hidden.shape
    depth = last_out.shape[1]
    index = w_out.shape[1] // depth - 1
    whole = pl.BlockSpec((rows, width), lambda i: (0, 0))
    return pl.pallas_call(
        final_kernel,
        grid=(1,),
        in_specs=[pl.BlockSpec((rows, depth), lambda i: (0, 0)), pl.BlockSpec((1, depth, width), lambda i: (layer, index, 0)), whole, whole],
        out_specs=whole,
        out_shape=jax.ShapeDtypeStruct((rows, width), jnp.bfloat16),
        scratch_shapes=[pltpu.VMEM((rows, width), jnp.float32)],
        name="final_update",
    )(last_out, w_out, sofar, hidden)


def flash_kernel(num_dev, which, q_ref, kv_hbm, out_ref, kv_buf, acc, m_s, l_s, s_a, s_b, sems):
    nch = kv_buf.shape[0]
    me = lax.axis_index("cp")
    half = q_ref.shape[1] // 2
    head = q_ref.shape[2]
    scale = head ** -0.5 * LOG2E
    num_rows = q_ref.shape[1]
    step_keys = kv_buf.shape[2]
    blocks = (me, 2 * num_dev - 1 - me)
    need = [(b * half + half + step_keys - 1) // step_keys for b in blocks]
    copies=lambda c: pltpu.make_async_copy(kv_hbm.at[c, which], kv_buf.at[c], sems.at[c])

    def start(c, carry):
        copies(c).start(); return carry

    lax.fori_loop(0, need[1], start, 0)
    m_s[...] = jnp.full(m_s.shape, NEG_BIG, jnp.float32)
    l_s[...] = jnp.zeros(l_s.shape, jnp.float32)
    acc[...] = jnp.zeros(acc.shape, jnp.float32)
    total = num_dev + 1

    def where(t):
        trail = t < need[1]
        b = jnp.where(trail, 1, 0)
        c = jnp.where(trail, t, t - need[1])
        return b, jnp.minimum(c, nch - 1)

    def qk(t, dst):
        b, c = where(t)
        dst[...] = lax.dot_general(q_ref[b], kv_buf[c, 0], NT, preferred_element_type=jnp.float32) * scale

    def soft(t, src, nxt, dst, masked):
        if dst is not None:
            qk(nxt, dst)
        b, c = where(t)
        s = src[...]
        if masked:
            row = jnp.where(b == 1, blocks[1], blocks[0]) * half + lax.rem(iota2((num_rows, step_keys), 0), half)
            key = c * step_keys + iota2((num_rows, step_keys), 1)
            s = jnp.where(key <= row, s, NEG_BIG)
        old = m_s[b]
        top = jnp.maximum(old, jnp.max(s, axis=-1, keepdims=True))
        e = jnp.exp2(s - jnp.concatenate([top] * (step_keys // 128), axis=1))
        fix = jnp.exp2(old - top)
        m_s[b] = top
        part = e[:, 0:128]
        for i in range(1, step_keys // 128):
            part = part + e[:, i * 128:(i + 1) * 128]
        l_s[b] = l_s[b] * fix + part
        acc[b] = acc[b] * jnp.concatenate([fix] * (head // 128), axis=1) + jnp.dot(e.astype(jnp.bfloat16), kv_buf[c, 1], preferred_element_type=jnp.float32)

    def tile(t, src, dst):
        nxt = t + 1

        @pl.when(nxt < need[1])
        def _():
            copies(nxt).wait()

        edge = jnp.logical_or(t == need[1] - 1, t == total - 1)

        @pl.when(edge)
        def _():
            soft(t, src, nxt, dst, True)

        @pl.when(jnp.logical_not(edge))
        def _():
            soft(t, src, nxt, dst, False)

    copies(0).wait()
    qk(0, s_a)

    def pair(u, carry):
        tile(2 * u, s_a, s_b)
        tile(2 * u + 1, s_b, s_a)
        return carry

    lax.fori_loop(0, (total - 1) // 2, pair, 0)
    soft(total - 1, s_a, None, None, True)
    for b in range(2):
        inv = 1.0 / jnp.sum(l_s[b],axis=-1,keepdims=True)
        out = (acc[b] * inv).astype(jnp.bfloat16)
        for g in range(2):
            out_ref[b * half:(b + 1) * half, g * head:(g + 1) * head] = out[g * half:(g + 1) * half]


def flash_head(queries, kv_all, which, num_dev):
    _, num_rows, head = queries.shape
    half = num_rows // 2
    f32 = jnp.float32
    nch, tok = kv_all.shape[0], kv_all.shape[3]
    return pl.pallas_call(
        functools.partial(flash_kernel, num_dev, which),
        out_shape=jax.ShapeDtypeStruct((2 * half, 2 * head), jnp.bfloat16),
        in_specs=[pl.BlockSpec(memory_space=pltpu.VMEM), pl.BlockSpec(memory_space=pltpu.HBM)],
        out_specs=pl.BlockSpec(memory_space=pltpu.VMEM),
        scratch_shapes=[pltpu.VMEM((nch, 2, tok, head), jnp.bfloat16), pltpu.VMEM((2, num_rows, head), f32),
            pltpu.VMEM((2, num_rows, 128), f32), pltpu.VMEM((2, num_rows, 128), f32), pltpu.VMEM((num_rows, tok), f32), pltpu.VMEM((num_rows, tok), f32), pltpu.SemaphoreType.DMA((nch,))],
        compiler_params=pltpu.CompilerParams(vmem_limit_bytes=48 * 1024 * 1024),
        cost_estimate=pl.CostEstimate(flops=20_000_000_000, bytes_accessed=16_000_000, transcendentals=0), name="flash_head")(queries, kv_all)


def output_owner(block_idx, num_dev):
    return block_idx if block_idx < num_dev else 2 * num_dev - 1 - block_idx


def to_output_layout(hidden, dev_rank, num_dev):
    block_len = hidden.shape[0] // 2
    even_pairs = [(source, output_owner(2 * source, num_dev)) for source in range(num_dev)]
    odd_pairs = [(source, output_owner(2 * source + 1, num_dev)) for source in range(num_dev)]
    from_even = lax.ppermute(hidden[:block_len], "cp", even_pairs)
    from_odd = lax.ppermute(hidden[block_len:], "cp", odd_pairs)
    is_even = dev_rank % 2 == 0
    lead_rows = jnp.where(is_even, from_even, from_odd)
    trail_rows = jnp.where(is_even, from_odd, from_even)
    return jnp.concatenate([lead_rows, trail_rows], axis=0)


def solution(mesh):
    num_dev = mesh.shape["cp"]

    def per_device(hidden, w_query, w_key, w_value, w_out):
        dev_rank = lax.axis_index("cp")
        layers, width, heads, head = w_query.shape
        kv_heads = w_key.shape[2]
        group = heads // kv_heads
        wo = w_out.reshape(layers, heads * head, width)
        last = layers - 1
        hidden, kv = local_layers(hidden, w_query, w_key, w_value, wo, num_dev, last)
        half = hidden.shape[0] // 2
        cuts = [0, kv_heads - 1, kv_heads]
        most = lax.all_gather(kv[:cuts[1]], "cp")
        rest = lax.all_gather(kv[cuts[1]:], "cp")
        hidden = to_output_layout(hidden, dev_rank, num_dev)
        gathered = [most, rest]
        normed = rms_normed(hidden).astype(jnp.bfloat16)
        queries = jnp.einsum("td,dhe->the", normed, w_query[last], preferred_element_type=jnp.float32).astype(jnp.bfloat16)
        queries = queries.reshape(2, half, kv_heads, group, head)
        outs = []
        for lo, hi, kv_all in zip(cuts, cuts[1:], gathered):
            for h in range(lo, hi):
                q = jnp.transpose(queries[:, :, h], (0, 2, 1, 3)).reshape(2, group * half, head)
                outs.append(flash_head(q, kv_all, h - lo, num_dev))
        return final_update(hidden, partial_update(outs[:-1], wo, last), outs[-1], wo, last)

    row_spec = P(("dp", "cp"), None)
    return jax.shard_map(per_device, mesh=mesh, in_specs=(row_spec, P(), P(), P(), P()), out_specs=row_spec, check_vma=False)
```

```python
import functools
import math

import jax
import jax.numpy as jnp
import numpy as np
from jax import lax
from jax.experimental import pallas as pl
from jax.experimental.pallas import tpu as pltpu
from jax.sharding import PartitionSpec as P


EPS_NORM = 1e-6
NEG_BIG = -1e30
LOG2E = 1.4426950408889634
MESH = pl.DeviceIdType.MESH
NT = (((1,), (1,)), ((), ()))


def rms_normed(rows_in):
    widened = rows_in.astype(jnp.float32)
    return widened * lax.rsqrt(jnp.mean(widened * widened, axis=-1, keepdims=True) + EPS_NORM)


def iota2(shape, dim):
    return lax.broadcasted_iota(jnp.int32, shape, dim)


def perm_matrix(heads):
    dn = 128 // heads
    row = np.arange(256)
    h, ct, d = row // (2 * dn), (row // dn) % 2, row % dn
    out = np.zeros((256, 256), np.float32)
    out[row, d * 2 * heads + ct * heads + h] = 1
    return jnp.asarray(out, jnp.bfloat16)


def local_kernel(num_dev, num_layers, x_hbm, wq_hbm, wk_hbm, wv_hbm, wo_hbm, perm_q, perm_k, x_out, own_s,
                 n_s, q_s, halo_a, halo_b, o_s, acc, w_s, raw, wo_buf, relay_1, relay_2, s_a, s_b,
                 x_sem, raw_sem, o_sem, send_a, send_b, recv_a, recv_b, send_r, recv_r, credit_a, credit_b, credit_r, credit_t):
    me = lax.axis_index("cp")
    odd = lax.rem(me, 2) == 1
    partner = jnp.where(odd, me - 1, me + 1)
    fwd = lax.rem(me + 2, num_dev)
    back = lax.rem(me + num_dev - 2, num_dev)
    ring = math.isqrt(num_dev // 2)
    chips = num_dev // 2
    chip, core = me // 2, lax.rem(me, 2)

    def ring_dev(c, shift):
        base = c // ring * ring
        return 2 * (base + lax.rem(c - base + ring + shift, ring)) + core

    left, right = ring_dev(chip, -1), ring_dev(chip, 1)
    target = 2 * lax.rem(ring_dev(chip, 2) // 2 + 1, chips) + core
    writer = ring_dev(lax.rem(chip + chips - 1, chips), -2)
    rows, width = n_s.shape
    half = rows // 2
    kv_heads = own_s.shape[0]
    relayed = kv_heads - 1
    heads = 2 * kv_heads
    head = own_s.shape[-1]
    scale = head ** -0.5 * LOG2E
    slots, raw_rows, lanes = raw.shape
    dq, dk = raw_rows // (2 * heads), raw_rows // (2 * kv_heads)
    kv_chunks, q_chunks = 2 * width // dk, width // dq
    span = kv_chunks + q_chunks
    total_chunks = span * num_layers + kv_chunks

    barrier = pltpu.get_barrier_semaphore()
    for other in (fwd, back, partner, left, right, target, writer):
        pl.semaphore_signal(barrier, inc=1, device_id={"cp": other}, device_id_type=MESH)
    pl.semaphore_wait(barrier, 7)

    def raw_copy(src, layer, i, g):
        slot = lax.rem(g, slots)
        part = pl.ds(pl.multiple_of(i * raw_rows, raw_rows), raw_rows)
        return pltpu.make_async_copy(src.at[layer, part], raw.at[slot], raw_sem.at[slot])

    def start_chunk(g):
        layer, i = g // span, lax.rem(g, span)

        @pl.when(jnp.logical_and(g < total_chunks, i < kv_chunks // 2))
        def _():
            raw_copy(wk_hbm, layer, i, g).start()

        @pl.when(jnp.logical_and(g < total_chunks, jnp.logical_and(i >= kv_chunks // 2, i < kv_chunks)))
        def _():
            raw_copy(wv_hbm, layer, i - kv_chunks // 2, g).start()

        @pl.when(jnp.logical_and(g < total_chunks, i >= kv_chunks))
        def _():
            raw_copy(wq_hbm, layer, i - kv_chunks, g).start()

    def flatten_chunk(layer, i, is_q):
        g = layer * span + i + (kv_chunks if is_q else 0)
        slot = lax.rem(g, slots)
        raw_copy(wk_hbm, 0, 0, g).wait()
        perm = perm_q if is_q else perm_k
        planes = heads if is_q else kv_heads
        dn = lanes // planes
        base = i * dq if is_q else lax.rem(i, kv_chunks // 2) * dk
        shift = 0 if is_q else pl.multiple_of(i // (kv_chunks // 2) * head, head)
        for b in range(raw_rows // 512):
            pair = jnp.concatenate([raw[slot, b * 512:b * 512 + 256, :], raw[slot, b * 512 + 256:b * 512 + 512, :]], axis=1)
            moved = jnp.dot(perm[...], pair, preferred_element_type=jnp.float32).astype(jnp.bfloat16)
            for h in range(planes):
                for ct in range(2):
                    row = (h * 2 + ct) * dn
                    for k in range(2):
                        part = pl.ds(pl.multiple_of(base + (2 * b + k) * dn, dn), dn)
                        piece = moved[row:row + dn, k * lanes:(k + 1) * lanes]
                        if is_q:
                            col = h % 2 * head + ct * lanes
                            w_s[h // 2, part, col:col + lanes] = piece
                        else:
                            w_s[h, part, pl.ds(pl.multiple_of(shift + ct * lanes, lanes), lanes)] = piece
        start_chunk(g + slots)

    def head_at(i):
        return jnp.where(i < kv_heads - 2, i, 2 * kv_heads - 3 - i)

    def o_copy(layer, i):
        slot = lax.rem(i, 2)
        part = pl.ds(pl.multiple_of(head_at(i) * 2 * head, 2 * head), 2 * head)
        dst = wo_buf.at[pl.ds(pl.multiple_of(slot * 2 * head, 2 * head), 2 * head)]
        return pltpu.make_async_copy(wo_hbm.at[layer, part], dst, o_sem.at[slot])

    x_copy = pltpu.make_async_copy(x_hbm, x_out, x_sem)
    x_copy.start()
    for g in range(slots):
        start_chunk(jnp.int32(g))
    for i in range(2):
        o_copy(0, jnp.int32(i)).start()

    def send_own(parity, h):
        return pltpu.make_async_remote_copy(
            src_ref=own_s.at[h], dst_ref=halo_a.at[parity, h], send_sem=send_a.at[h], recv_sem=recv_a.at[parity, h],
            device_id={"cp": fwd}, device_id_type=MESH)

    def send_partner(parity, h, src):
        return pltpu.make_async_remote_copy(
            src_ref=src, dst_ref=halo_b.at[parity, h], send_sem=send_b.at[h], recv_sem=recv_b.at[parity, h],
            device_id={"cp": partner}, device_id_type=MESH)

    def hop(parity, leg, kv):
        src = (own_s.at[relayed, kv], relay_1.at[parity, kv], relay_2.at[parity, kv])[leg]
        dst = (relay_1.at[parity, kv], relay_2.at[parity, kv], halo_a.at[parity, relayed, kv])[leg]
        return pltpu.make_async_remote_copy(
            src_ref=src, dst_ref=dst, send_sem=send_r.at[leg, kv], recv_sem=recv_r.at[parity, leg, kv],
            device_id={"cp": (left, left, target)[leg]}, device_id_type=MESH)

    def pass_on(parity, leg, kv):
        hop(parity, leg, kv).wait_recv()
        hop(parity, leg + 1, kv).start()

    def flatten_range(layer, lo, hi, is_q):
        def one(i, c):
            flatten_chunk(layer, i, is_q)
            return c

        lax.fori_loop(lo, hi, one, 0)

    x_copy.wait()

    def norm_rows(i, carry):
        part = pl.ds(pl.multiple_of(i * 64, 64), 64)
        n_s[part, :] = rms_normed(x_out[part, :]).astype(jnp.bfloat16)
        return carry

    lax.fori_loop(0, rows // 64, norm_rows, 0)
    flatten_range(0, 0, kv_chunks, False)

    bias_a = jnp.where(me < 2, NEG_BIG, 0.0)
    bias_b = jnp.where(me < 1, NEG_BIG, 0.0)

    def attend(parity, h, slot):
        row, key = iota2((half, half), 0), iota2((half, half), 1)
        units = [(j, g, (s_a, s_b)[j].at[g * half:(g + 1) * half]) for j in range(2) for g in range(2)]

        def blocks_of(j):
            return [(halo_a.at[parity, h], 0, bias_a), (halo_a.at[parity, h], 1, bias_a),
                    (halo_b.at[parity, h], 0, bias_b), (halo_b.at[parity, h], 1, bias_b),
                    (own_s.at[h], 0, None), (own_s.at[h], 1, None)][j:j + 5]

        def score(j, g, buf):
            q_tile = q_s[h, j, g * half:(g + 1) * half, :]
            for i, (ref, part, bias) in enumerate(blocks_of(j)):
                keys = ref[0, part * half:(part + 1) * half, :]
                scores = lax.dot_general(q_tile, keys, NT, preferred_element_type=jnp.float32) * scale
                if bias is not None:
                    scores = scores + bias
                if i == 0:
                    scores = jnp.where(key > row, scores, NEG_BIG)
                if i == 4:
                    scores = jnp.where(key <= row, scores, NEG_BIG)
                buf[:, i * half:(i + 1) * half] = scores

        score(*units[0])
        for u, (j, g, buf) in enumerate(units):
            if u + 1 < len(units):
                score(*units[u + 1])
            tiles = [buf[:, i * half:(i + 1) * half] for i in range(5)]
            top = jnp.max(functools.reduce(jnp.maximum, tiles), axis=-1, keepdims=True)
            total, out = None, None
            for scores, (ref, part, _) in zip(tiles, blocks_of(j)):
                e = jnp.exp2(scores - top)
                total = e if total is None else total + e
                term = jnp.dot(e.astype(jnp.bfloat16), ref[1, part * half:(part + 1) * half, :], preferred_element_type=jnp.float32)
                out = term if out is None else out + term
            out = (out / jnp.sum(total, axis=-1, keepdims=True)).astype(jnp.bfloat16)
            cols = pl.ds(pl.multiple_of(slot * 2 * head + g * head, head), head)
            o_s[j * half:(j + 1) * half, cols] = out

    def project_kv(h):
        kv = jnp.dot(n_s[...], w_s[h], preferred_element_type=jnp.float32).astype(jnp.bfloat16)
        own_s[h, 0] = kv[:, 0:head]
        own_s[h, 1] = kv[:, head:2 * head]

    def layer_step(layer, carry):
        parity = lax.rem(layer, 2)

        @pl.when(layer >= 2)
        def _():
            pl.semaphore_wait(credit_a, 1)
            pl.semaphore_wait(credit_b, 1)
            pl.semaphore_wait(credit_r, 1)
            pl.semaphore_wait(credit_t, 1)

        def kv_step(i, c):
            h = lax.rem(i + relayed, kv_heads)
            project_kv(h)

            @pl.when(h == relayed)
            def _():
                hop(parity, 0, 0).start()
                hop(parity, 0, 1).start()

            @pl.when(h != relayed)
            def _():
                send_own(parity, h).start()

            @pl.when(jnp.logical_not(odd))
            def _():
                send_partner(parity, h, own_s.at[h]).start()

            return c

        lax.fori_loop(0, kv_heads, kv_step, 0)

        def flatten_q(t, c):
            flatten_range(layer, t * q_chunks // 2, (t + 1) * q_chunks // 2, True)

            @pl.when(t == 0)
            def _():
                pass_on(parity, 0, 0)

            return c

        lax.fori_loop(0, 2, flatten_q, 0)

        def q_step(h, c):
            @pl.when(h == 1)
            def _():
                pass_on(parity, 0, 1)

            @pl.when(h == kv_heads - 1)
            def _():
                pass_on(parity, 1, 0)

            q = jnp.dot(n_s[...], w_s[h], preferred_element_type=jnp.float32).astype(jnp.bfloat16)
            for g in range(2):
                for j in range(2):
                    q_s[h, j, g * half:(g + 1) * half, :] = q[j * half:(j + 1) * half, g * head:(g + 1) * head]
            return c

        lax.fori_loop(0, kv_heads, q_step, 0)

        def attn_step(i, c):
            slot, h = lax.rem(i, 2), head_at(i)

            @pl.when(i == 1)
            def _():
                pass_on(parity, 1, 1)

            early = kv_chunks * 4 // 5
            flatten_range(layer + 1, jnp.where(i == kv_heads - 1, early, kv_chunks), kv_chunks, False)

            @pl.when(h == relayed)
            def _():
                hop(parity, 2, 0).wait_recv()
                hop(parity, 2, 1).wait_recv()

            @pl.when(h != relayed)
            def _():
                send_own(parity, h).wait_recv()

            @pl.when(odd)
            def _():
                send_partner(parity, h, halo_a.at[parity, h]).start()

            flatten_range(layer + 1, jnp.minimum(i * early // (kv_heads - 1), early), jnp.minimum((i + 1) * early // (kv_heads - 1), early), False)
            send_partner(parity, h, own_s.at[h]).wait_recv()
            attend(parity, h, slot)

            @pl.when(slot == 1)
            def _():
                o_copy(layer, i - 1).wait()
                o_copy(layer, i).wait()
                block = width // 2

                def out_part(t, cc):
                    cols = pl.ds(pl.multiple_of(t * block, block), block)
                    part = jnp.dot(o_s[...], wo_buf[:, cols], preferred_element_type=jnp.float32)

                    @pl.when(i == 1)
                    def _():
                        acc[:, cols] = part

                    @pl.when(i > 1)
                    def _():
                        acc[:, cols] = acc[:, cols] + part

                    return cc

                lax.fori_loop(0, 2, out_part, 0)

                @pl.when(i < kv_heads - 2)
                def _():
                    o_copy(layer, i + 1).start()
                    o_copy(layer, i + 2).start()

                @pl.when(jnp.logical_and(i >= kv_heads - 2, layer < num_layers - 1))
                def _():
                    o_copy(layer + 1, i + 1 - kv_heads).start()
                    o_copy(layer + 1, i + 2 - kv_heads).start()

            return c

        lax.fori_loop(0, kv_heads, attn_step, 0)

        def drain(h, c):
            @pl.when(h != relayed)
            def _():
                send_own(parity, h).wait_send()

            send_partner(parity, h, own_s.at[h]).wait_send()
            return c

        lax.fori_loop(0, kv_heads, drain, 0)
        for leg in range(3):
            for kv in range(2):
                hop(parity, leg, kv).wait_send()

        @pl.when(layer < num_layers - 2)
        def _():
            pl.semaphore_signal(credit_a, inc=1, device_id={"cp": back}, device_id_type=MESH)
            pl.semaphore_signal(credit_b, inc=1, device_id={"cp": partner}, device_id_type=MESH)
            pl.semaphore_signal(credit_r, inc=1, device_id={"cp": right}, device_id_type=MESH)
            pl.semaphore_signal(credit_t, inc=1, device_id={"cp": writer}, device_id_type=MESH)

        def update_rows(i, c):
            part = pl.ds(pl.multiple_of(i * 64, 64), 64)
            fresh = (x_out[part, :].astype(jnp.float32) + rms_normed(acc[part, :])).astype(jnp.bfloat16)
            x_out[part, :] = fresh
            n_s[part, :] = rms_normed(fresh).astype(jnp.bfloat16)
            return c

        lax.fori_loop(0, rows // 64, update_rows, 0)
        return carry

    lax.fori_loop(0, num_layers, layer_step, 0)

    def last_kv(h, c):
        project_kv(h)
        return c

    lax.fori_loop(0, kv_heads, last_kv, 0)


def tile_rows(w):
    layers, width, heads, _ = w.shape
    return w.reshape(layers, width, heads, 2, 128).transpose(0, 1, 3, 2, 4).reshape(layers, width * 2 * heads, 128)


def local_layers(hidden, w_query, w_key, w_value, w_out, num_dev, num_layers):
    rows, width = hidden.shape
    heads, head = w_query.shape[2:]
    kv_heads = w_key.shape[2]
    half = rows // 2
    bf16, f32 = jnp.bfloat16, jnp.float32
    hbm = pl.BlockSpec(memory_space=pltpu.HBM)
    vmem = pl.BlockSpec(memory_space=pltpu.VMEM)
    dma = pltpu.SemaphoreType.DMA
    return pl.pallas_call(
        functools.partial(local_kernel, num_dev, num_layers),
        out_shape=(jax.ShapeDtypeStruct((rows, width), bf16), jax.ShapeDtypeStruct((kv_heads, 2, rows, head), bf16)),
        in_specs=[hbm, hbm, hbm, hbm, hbm, vmem, vmem],
        out_specs=(vmem, vmem),
        scratch_shapes=[
            pltpu.VMEM((rows, width), bf16),
            pltpu.VMEM((kv_heads, 2, 2 * half, head), bf16),
            pltpu.VMEM((2, kv_heads, 2, rows, head), bf16),
            pltpu.VMEM((2, kv_heads, 2, rows, head), bf16),
            pltpu.VMEM((rows, 4 * head), bf16),
            pltpu.VMEM((rows, width), f32),
            pltpu.VMEM((kv_heads, width, 2 * head), bf16),
            pltpu.VMEM((4, 4096, 128), bf16),
            pltpu.VMEM((4 * head, width), bf16),
            pltpu.VMEM((2, 2, rows, head), bf16),
            pltpu.VMEM((2, 2, rows, head), bf16),
            pltpu.VMEM((2 * half, 5 * half), f32),
            pltpu.VMEM((2 * half, 5 * half), f32),
            dma, dma((4,)), dma((2,)),
            dma((kv_heads,)), dma((kv_heads,)), dma((2, kv_heads)), dma((2, kv_heads)), dma((3, 2)), dma((2, 3, 2)),
            pltpu.SemaphoreType.REGULAR, pltpu.SemaphoreType.REGULAR, pltpu.SemaphoreType.REGULAR, pltpu.SemaphoreType.REGULAR,
        ],
        compiler_params=pltpu.CompilerParams(collective_id=0, has_side_effects=True, vmem_limit_bytes=62 * 1024 * 1024),
        name="local_layers",
    )(hidden, tile_rows(w_query), tile_rows(w_key), tile_rows(w_value), w_out, perm_matrix(heads), perm_matrix(kv_heads))


def partial_kernel(count, *refs):
    attn, w, out = refs[:count], refs[count], refs[count + 1]
    for i in range(count):
        @pl.when(pl.program_id(0) == i)
        def _(i=i):
            part = jnp.dot(attn[i][...], w[0], preferred_element_type=jnp.float32)
            out[...] = part if i == 0 else out[...] + part


def final_kernel(attn, w, sofar, x, out, acc):
    acc[...] = sofar[...] + jnp.dot(attn[...], w[0], preferred_element_type=jnp.float32)

    def one(i, c):
        part = pl.ds(pl.multiple_of(i * 64, 64), 64)
        out[part, :] = (x[part, :].astype(jnp.float32) + rms_normed(acc[part, :])).astype(jnp.bfloat16)
        return c

    lax.fori_loop(0, out.shape[0] // 64, one, 0)


def partial_update(outs, w_out, layer):
    rows, depth = outs[0].shape
    width = w_out.shape[2]
    count = len(outs)
    return pl.pallas_call(
        functools.partial(partial_kernel, count),
        grid=(count,),
        in_specs=[pl.BlockSpec((rows, depth), lambda i: (0, 0))] * count + [pl.BlockSpec((1, depth, width), lambda i: (layer, i, 0))],
        out_specs=pl.BlockSpec((rows, width), lambda i: (0, 0)),
        out_shape=jax.ShapeDtypeStruct((rows, width), jnp.float32),
        cost_estimate=pl.CostEstimate(flops=2 * count * rows * depth * width, bytes_accessed=16_000_000, transcendentals=0),
        name="partial_update",
    )(*outs, w_out)


def final_update(hidden, sofar, last_out, w_out, layer):
    rows, width = hidden.shape
    depth = last_out.shape[1]
    index = w_out.shape[1] // depth - 1
    whole = pl.BlockSpec((rows, width), lambda i: (0, 0))
    return pl.pallas_call(
        final_kernel,
        grid=(1,),
        in_specs=[pl.BlockSpec((rows, depth), lambda i: (0, 0)), pl.BlockSpec((1, depth, width), lambda i: (layer, index, 0)), whole, whole],
        out_specs=whole,
        out_shape=jax.ShapeDtypeStruct((rows, width), jnp.bfloat16),
        scratch_shapes=[pltpu.VMEM((rows, width), jnp.float32)],
        name="final_update",
    )(last_out, w_out, sofar, hidden)


def flash_kernel(num_dev, which, q_ref, kv_hbm, out_ref, kv_buf, acc, m_s, l_s, s_a, s_b, sems):
    nch = kv_buf.shape[0]
    me = lax.axis_index("cp")
    half = q_ref.shape[1] // 2
    head = q_ref.shape[2]
    scale = head ** -0.5 * LOG2E
    num_rows = q_ref.shape[1]
    step_keys = kv_buf.shape[2]
    blocks = (me, 2 * num_dev - 1 - me)
    need = [(b * half + half + step_keys - 1) // step_keys for b in blocks]
    copies=lambda c: pltpu.make_async_copy(kv_hbm.at[c, which], kv_buf.at[c], sems.at[c])

    def start(c, carry):
        copies(c).start(); return carry

    lax.fori_loop(0, need[1], start, 0)
    m_s[...] = jnp.full(m_s.shape, NEG_BIG, jnp.float32)
    l_s[...] = jnp.zeros(l_s.shape, jnp.float32)
    acc[...] = jnp.zeros(acc.shape, jnp.float32)
    total = num_dev + 1

    def where(t):
        trail = t < need[1]
        b = jnp.where(trail, 1, 0)
        c = jnp.where(trail, t, t - need[1])
        return b, jnp.minimum(c, nch - 1)

    def qk(t, dst):
        b, c = where(t)
        dst[...] = lax.dot_general(q_ref[b], kv_buf[c, 0], NT, preferred_element_type=jnp.float32) * scale

    def soft(t, src, nxt, dst, masked):
        if dst is not None:
            qk(nxt, dst)
        b, c = where(t)
        s = src[...]
        if masked:
            row = jnp.where(b == 1, blocks[1], blocks[0]) * half + lax.rem(iota2((num_rows, step_keys), 0), half)
            key = c * step_keys + iota2((num_rows, step_keys), 1)
            s = jnp.where(key <= row, s, NEG_BIG)
        old = m_s[b]
        top = jnp.maximum(old, jnp.max(s, axis=-1, keepdims=True))
        e = jnp.exp2(s - jnp.concatenate([top] * (step_keys // 128), axis=1))
        fix = jnp.exp2(old - top)
        m_s[b] = top
        part = e[:, 0:128]
        for i in range(1, step_keys // 128):
            part = part + e[:, i * 128:(i + 1) * 128]
        l_s[b] = l_s[b] * fix + part
        acc[b] = acc[b] * jnp.concatenate([fix] * (head // 128), axis=1) + jnp.dot(e.astype(jnp.bfloat16), kv_buf[c, 1], preferred_element_type=jnp.float32)

    def tile(t, src, dst):
        nxt = t + 1

        @pl.when(nxt < need[1])
        def _():
            copies(nxt).wait()

        edge = jnp.logical_or(t == need[1] - 1, t == total - 1)

        @pl.when(edge)
        def _():
            soft(t, src, nxt, dst, True)

        @pl.when(jnp.logical_not(edge))
        def _():
            soft(t, src, nxt, dst, False)

    copies(0).wait()
    qk(0, s_a)

    def pair(u, carry):
        tile(2 * u, s_a, s_b)
        tile(2 * u + 1, s_b, s_a)
        return carry

    lax.fori_loop(0, (total - 1) // 2, pair, 0)
    soft(total - 1, s_a, None, None, True)
    for b in range(2):
        inv = 1.0 / jnp.sum(l_s[b],axis=-1,keepdims=True)
        out = (acc[b] * inv).astype(jnp.bfloat16)
        for g in range(2):
            out_ref[b * half:(b + 1) * half, g * head:(g + 1) * head] = out[g * half:(g + 1) * half]


def flash_head(queries, kv_all, which, num_dev):
    _, num_rows, head = queries.shape
    half = num_rows // 2
    f32 = jnp.float32
    nch, tok = kv_all.shape[0], kv_all.shape[3]
    return pl.pallas_call(
        functools.partial(flash_kernel, num_dev, which),
        out_shape=jax.ShapeDtypeStruct((2 * half, 2 * head), jnp.bfloat16),
        in_specs=[pl.BlockSpec(memory_space=pltpu.VMEM), pl.BlockSpec(memory_space=pltpu.HBM)],
        out_specs=pl.BlockSpec(memory_space=pltpu.VMEM),
        scratch_shapes=[pltpu.VMEM((nch, 2, tok, head), jnp.bfloat16), pltpu.VMEM((2, num_rows, head), f32),
            pltpu.VMEM((2, num_rows, 128), f32), pltpu.VMEM((2, num_rows, 128), f32), pltpu.VMEM((num_rows, tok), f32), pltpu.VMEM((num_rows, tok), f32), pltpu.SemaphoreType.DMA((nch,))],
        compiler_params=pltpu.CompilerParams(vmem_limit_bytes=48 * 1024 * 1024),
        cost_estimate=pl.CostEstimate(flops=20_000_000_000, bytes_accessed=16_000_000, transcendentals=0), name="flash_head")(queries, kv_all)


def output_owner(block_idx, num_dev):
    return block_idx if block_idx < num_dev else 2 * num_dev - 1 - block_idx


def to_output_layout(hidden, dev_rank, num_dev):
    block_len = hidden.shape[0] // 2
    even_pairs = [(source, output_owner(2 * source, num_dev)) for source in range(num_dev)]
    odd_pairs = [(source, output_owner(2 * source + 1, num_dev)) for source in range(num_dev)]
    from_even = lax.ppermute(hidden[:block_len], "cp", even_pairs)
    from_odd = lax.ppermute(hidden[block_len:], "cp", odd_pairs)
    is_even = dev_rank % 2 == 0
    lead_rows = jnp.where(is_even, from_even, from_odd)
    trail_rows = jnp.where(is_even, from_odd, from_even)
    return jnp.concatenate([lead_rows, trail_rows], axis=0)


def solution(mesh):
    num_dev = mesh.shape["cp"]

    def per_device(hidden, w_query, w_key, w_value, w_out):
        dev_rank = lax.axis_index("cp")
        layers, width, heads, head = w_query.shape
        kv_heads = w_key.shape[2]
        group = heads // kv_heads
        wo = w_out.reshape(layers, heads * head, width)
        last = layers - 1
        hidden, kv = local_layers(hidden, w_query, w_key, w_value, wo, num_dev, last)
        half = hidden.shape[0] // 2
        cuts = [0, kv_heads - 1, kv_heads]
        most = lax.all_gather(kv[:cuts[1]], "cp")
        rest = lax.all_gather(kv[cuts[1]:], "cp")
        hidden = to_output_layout(hidden, dev_rank, num_dev)
        gathered = [most, rest]
        normed = rms_normed(hidden).astype(jnp.bfloat16)
        queries = jnp.einsum("td,dhe->the", normed, w_query[last], preferred_element_type=jnp.float32).astype(jnp.bfloat16)
        queries = queries.reshape(2, half, kv_heads, group, head)
        outs = []
        for lo, hi, kv_all in zip(cuts, cuts[1:], gathered):
            for h in range(lo, hi):
                q = jnp.transpose(queries[:, :, h], (0, 2, 1, 3)).reshape(2, group * half, head)
                outs.append(flash_head(q, kv_all, h - lo, num_dev))
        return final_update(hidden, partial_update(outs[:-1], wo, last), outs[-1], wo, last)

    row_spec = P(("dp", "cp"), None)
    return jax.shard_map(per_device, mesh=mesh, in_specs=(row_spec, P(), P(), P(), P()), out_specs=row_spec, check_vma=False)
```
